256 devices in a mesh: row: 32 (over x, y, core), col: 8 (over z).
Axes of the slice: x: 4, y: 4, z: 8, core: 2. Of those that a mesh axis runs over, the one named last changes fastest.
Arguments:
- hidden: bfloat16 [64, 6144], P('col', 'row'), may hold values from -6 to 6
- queries: bfloat16 [64, 6144], P('row', 'col'), may hold values from -48 to 48
- new_keys: bfloat16 [64, 1024], P('row', 'col'), may hold values from -4 to 4
- new_values: bfloat16 [64, 1024], P('row', 'col'), may hold values from -6 to 6
- cache_keys: bfloat16 [64, 2048, 1024], P('row', None, 'col'), may hold values from -6 to 6
- cache_values: bfloat16 [64, 2048, 1024], P('row', None, 'col'), may hold values from -6 to 6
- lengths: int32 [64], P('row'), may hold values from 1 to 2048, 65536 in all
- page_table: int32 [64, 8], replicated, may hold values from 0 to 63
- resident: int32 [32, 4], replicated, may hold values from 0 to 63, as said below
- prefix_keys: bfloat16 [32, 4, 128, 1024], P('row', None, None, 'col'), may hold values from -4 to 4, as said below
- prefix_values: bfloat16 [32, 4, 128, 1024], P('row', None, None, 'col'), may hold values from -16 to 16, as said below
- out_weight: bfloat16 [6144, 6144], P('col', 'row'), may hold values from -0.078125 to 0.078125
- norm_gain: float32 [6144], P('row'), may hold values from 0.5 to 1.5
- router_weight: bfloat16 [6144, 8], P('row'), may hold values from -0.078125 to 0.078125
- experts: int32 [64, 2], P('col'), may hold values from 0 to 7, all different within a row; in each aligned block of 8 rows (0 to 7, 8 to 15, ...) at most 4 rows name the same one
- gate_weight: bfloat16 [8, 6144, 8192], P('col', None, 'row'), may hold values from -0.078125 to 0.078125
- up_weight: bfloat16 [8, 6144, 8192], P('col', None, 'row'), may hold values from -0.078125 to 0.078125
- down_projection_weight: bfloat16 [8, 8192, 6144], P('col', 'row'), may hold values from -0.0625 to 0.0625
Outputs:
- layer_out: bfloat16 [64, 6144], P('col', 'row')
The draws below stay inside these ranges and needn't reach their ends.
Inputs may be any that keep to these rules, and one draw needn't show every extreme that they name: `resident`: each row's 4 slots hold different page ids, and every id below 64 is held by at least one row. `prefix_keys`: slots holding the same page id hold the same keys, on every row. `prefix_values`: slots holding the same page id hold the same values, on every row. The two experts of a token differ; in each aligned block of 8 tokens at most 4 tokens name the same expert.
All inputs are finite; a program needn't handle non-finite values. No bound on the sum of `lengths` on one device may be relied on, other than what follows from the above.
Results may differ from the reference program's by a relative error of at most 0.0095.
Values may be sent and summed in bfloat16 or wider, within the bound.
A program may use at most 128 MiB of HBM per device.

```python
import math
import jax
import jax.numpy as jnp
import numpy as np
from jax import lax

D = 6144
HQ = 48
KVH = 8
HD = 128
EXPERT_COUNT = 8
EXPERTS_PER_TOKEN = 2
FFW = 8192
PAGE = 128
MAXP = 8
SLOTS = 4
PRE_HOME = 2
SEQS = 64
TOK_COL = 8
CAP = 4
CTX = 2048
NPRE = 64
N_ROW = 32
N_COL = 8


def fresh_draw(key):
    base = jnp.clip(jax.random.normal(key, (SEQS, KVH * HD), jnp.float32), -4.0, 4.0)
    return base


def residency(key):
    npages = PRE_HOME * N_ROW
    extra = SLOTS - PRE_HOME
    rows = jnp.arange(N_ROW, dtype=jnp.int32)
    home = rows[:, None] * PRE_HOME + jnp.arange(PRE_HOME, dtype=jnp.int32)[None, :]

    def pick_others(subkey):
        return jax.random.permutation(subkey, npages - PRE_HOME)[:extra].astype(jnp.int32)

    def shuffle_slots(subkey):
        return jax.random.permutation(subkey, SLOTS).astype(jnp.int32)
    offsets = jax.vmap(pick_others)(jax.random.split(jax.random.fold_in(key, 1), N_ROW))
    others = (rows[:, None] * PRE_HOME + PRE_HOME + offsets) % npages
    ids = jnp.concatenate([home, others], axis=1).astype(jnp.int32)
    relabel = jax.random.permutation(jax.random.fold_in(key, 2), npages).astype(jnp.int32)
    ids = relabel[ids]
    order = jax.vmap(shuffle_slots)(jax.random.split(jax.random.fold_in(key, 3), N_ROW))
    return jnp.take_along_axis(ids, order, axis=1).astype(jnp.int32)


def page_contents(key, factor):
    npages = PRE_HOME * N_ROW
    pages = jnp.clip(jax.random.normal(key, (npages, PAGE, KVH * HD), jnp.float32), -4.0, 4.0)
    return pages * factor


def draw_new_keys(key, part):
    return fresh_draw(jax.random.fold_in(key, 5)).astype(jnp.bfloat16)


def draw_queries(key, part):
    base = jnp.clip(jax.random.normal(jax.random.fold_in(key, 6), (SEQS, HQ * HD), jnp.float32), -4.0, 4.0)
    return base.astype(jnp.bfloat16)


def draw_resident(key, part):
    return residency(jax.random.fold_in(key, 40))


def draw_prefix_keys(key, part):
    ids = residency(jax.random.fold_in(key, 40))
    pages = page_contents(jax.random.fold_in(key, 41), 1.0)
    return pages[ids].astype(jnp.bfloat16)


def draw_prefix_values(key, part):
    ids = residency(jax.random.fold_in(key, 40))
    pages = page_contents(jax.random.fold_in(key, 42), 4.0)
    return pages[ids].astype(jnp.bfloat16)


def touch_ends(values, rng, smallest, high):
    dims = values.shape
    index_at = [jax.random.randint(jax.random.fold_in(rng, axis), (), 0, dims[axis]) for axis in range(len(dims))]
    values = values.at[tuple(index_at)].set(smallest)
    longest = dims.index(max(dims))
    index_at[longest] = (index_at[longest] + 1) % dims[longest]
    return values.at[tuple(index_at)].set(high)


def shard_levels(stream_key, shape, pieces, least, largest):
    def one(dim, parts):
        steps = jax.random.uniform(jax.random.fold_in(jax.random.fold_in(stream_key, 6), dim), (parts,), jnp.float32, least / len(pieces), largest / len(pieces))
        return jnp.repeat(jnp.exp(steps), shape[dim] // parts).reshape((-1,) + (1,) * (len(shape) - dim - 1))

    gain = one(*pieces[0])
    for cut in pieces[1:]:
        gain = gain * one(*cut)
    return gain


def cumulative_ranks(amount, skew):
    loads = [(1 << 20) // math.isqrt(standing ** skew) + 1 for standing in range(1, amount + 1)]
    width = 1 + sum(loads) // (1 << 30)
    return np.cumsum(np.array([max(1, weight // width) for weight in loads]))


def ranked_ids(rng, extent, amount, slope):
    listing = cumulative_ranks(amount, slope)
    lot = jax.random.randint(jax.random.fold_in(rng, 1), extent, 0, int(listing[amount - 1]))
    standing = jnp.searchsorted(jnp.asarray(listing, jnp.int32), lot, side="right")
    return jax.random.permutation(jax.random.fold_in(rng, 2), amount)[standing].astype(jnp.int32)


def split_up(count, total, most, slope):
    loads = [(1 << 20) // math.isqrt(standing ** slope) + 1 for standing in range(2, count + 1)]
    rest, counts = total - most - (count - 1), [1] * (count - 1)
    while rest > 0:
        free = [i for i in range(count - 1) if counts[i] < most]
        whole, budget = sum([loads[i] for i in free]), rest
        for i in free:
            more = min(most - counts[i], max(1, budget * loads[i] // whole), rest)
            counts[i] = counts[i] + more
            rest = rest - more
    return np.array([most] + counts)


def uneven(own_key, number_of, total, bound, skew):
    if number_of == 2:
        one = jax.random.randint(own_key, (), max(1, total - bound), min(bound, total - 1) + 1)
        return jnp.stack([one, total - one])
    sizes = jnp.asarray(split_up(number_of, total, bound, skew), jnp.int32)
    pairs = (number_of - 1) // 2
    giver, taker = sizes[1:1 + 2 * pairs:2], sizes[2:2 + 2 * pairs:2]
    room = jnp.minimum(giver - 1, bound - taker)
    passed = jax.random.randint(jax.random.fold_in(own_key, 1), (pairs,), 0, 1 << 20) % (room + 1)
    sizes = sizes.at[1:1 + 2 * pairs:2].set(giver - passed).at[2:2 + 2 * pairs:2].set(taker + passed)
    return sizes[jax.random.permutation(jax.random.fold_in(own_key, 2), number_of)]


def assign_block(stream_key, own, number, rows, number_of, top, most, lean):
    order = jax.random.permutation(stream_key, number_of)
    heavy_load, common = load_shares(number_of, rows * top, most, lean, True), load_shares(number_of, rows * top, most, lean, False)
    places = jnp.arange(number_of)

    def named(tallies, offset_by):
        used = int((tallies > 0).sum())
        fixed = max(1, used // 4)
        shifted = fixed + (places - fixed + offset_by * (used - fixed)) % max(1, number_of - fixed)
        return jnp.zeros((number_of,), jnp.int32).at[order[jnp.where(places < fixed, places, shifted)]].set(jnp.asarray(tallies, jnp.int32))

    tallies = jnp.where(number % 4 == 0, named(heavy_load, number // 4), named(common, number - number // 4 - 1))
    mixed = jax.random.permutation(jax.random.fold_in(own, 3), number_of)
    source_of, receiver = mixed[0:number_of // 2 * 2:2], mixed[1:number_of // 2 * 2:2]
    slack = jnp.minimum(tallies[source_of] - 1, most - tallies[receiver]) // 2
    slack = jnp.where((source_of == order[0]) | (receiver == order[0]) | (tallies[receiver] == 0), 0, jnp.maximum(slack, 0))
    shifted = jax.random.randint(jax.random.fold_in(own, 4), (number_of // 2,), 0, 1 << 20) % (slack + 1)
    tallies = tallies.at[source_of].add(-shifted).at[receiver].add(shifted)
    items = jnp.searchsorted(jnp.cumsum(tallies), jnp.arange(rows * top), side="right").astype(jnp.int32)
    grid = items.reshape(top, rows).T
    grid = grid[jax.random.permutation(jax.random.fold_in(own, 1), rows)]
    offset_by = jax.random.randint(jax.random.fold_in(own, 2), (rows, 1), 0, top)
    return jnp.take_along_axis(grid, (jnp.arange(top)[None, :] + offset_by) % top, axis=1)


def load_shares(number_of, total, reach, slope, full):
    loads = [(1 << 20) // math.isqrt(grade ** slope) + 1 for grade in range(1, number_of + 1)]
    largest = reach if full else min(reach, max(-(-total // number_of), total * loads[0] // sum(loads)))
    least = 1 if total - largest >= number_of - 1 else 0
    counts, spare = [largest] + [least] * (number_of - 1), total - largest - least * (number_of - 1)
    while spare > 0:
        candidates = [i for i in range(1, number_of) if counts[i] < largest] or [i for i in range(1, number_of) if counts[i] < reach]
        pool, left = sum([loads[i] for i in candidates]), spare
        for i in candidates:
            addition = min(reach - counts[i], max(1, left * loads[i] // pool), spare)
            counts[i] = counts[i] + addition
            spare = spare - addition
    return np.array(counts)


def scatter_about(stream_key, extent, width, limit, cuts=(), kind=jnp.bfloat16):
    factor_of = shard_levels(stream_key, extent, cuts, -0.22, 0.18) if cuts else 1.0
    result = jax.random.normal(stream_key, extent, jnp.float32) * width * factor_of
    return jnp.minimum(jnp.maximum(result, -limit), limit).astype(kind)


def setup_inputs(seed: int = 0) -> dict:
    key_of = jax.random.split(jax.random.key(seed), 19)
    hidden = scatter_about(key_of[0], (SEQS, D), 1.0, 6.0, ((0, 8), (1, 32)))
    queries = draw_queries(jax.random.fold_in(key_of[18], 71), 0)
    new_keys = draw_new_keys(jax.random.fold_in(key_of[18], 71), 0)
    new_values = scatter_about(key_of[3], (SEQS, KVH * HD), 1.0, 6.0, ((0, 32), (1, 8)))
    cache_keys = scatter_about(key_of[4], (SEQS, CTX, KVH * HD), 1.0, 6.0, ((0, 32), (2, 8)))
    cache_values = scatter_about(key_of[5], (SEQS, CTX, KVH * HD), 1.0, 6.0, ((0, 32), (2, 8)))
    lengths = uneven(key_of[6], SEQS, SEQS * CTX // 2, CTX, 2).astype(jnp.int32)
    page_table = touch_ends(ranked_ids(key_of[7], (SEQS, MAXP), NPRE, 2), jax.random.fold_in(key_of[7], 3), 0, NPRE - 1).astype(jnp.int32)
    resident = draw_resident(jax.random.fold_in(key_of[18], 71), 0)
    prefix_keys = draw_prefix_keys(jax.random.fold_in(key_of[18], 71), 0)
    prefix_values = draw_prefix_values(jax.random.fold_in(key_of[18], 71), 0)
    out_weight = scatter_about(key_of[11], (HQ * HD, D), (HQ * HD) ** -0.5, 0.078125, ((0, 8), (1, 32)))
    norm_gain = jnp.clip(1.0 + 0.1 * jax.random.normal(key_of[12], (D,), jnp.float32), 0.5, 1.5)
    router_weight = scatter_about(key_of[13], (D, EXPERT_COUNT), D ** -0.5, 0.078125, ((0, 32),))
    experts_keys = jax.random.split(jax.random.fold_in(key_of[14], 1), SEQS // TOK_COL)
    experts_turns = jax.random.permutation(jax.random.fold_in(key_of[14], 3), SEQS // TOK_COL)
    experts = jax.vmap(lambda own, number: assign_block(jax.random.fold_in(key_of[14], 2), own, number, TOK_COL, EXPERT_COUNT, EXPERTS_PER_TOKEN, CAP, 2))(experts_keys, experts_turns).reshape((SEQS, EXPERTS_PER_TOKEN))
    gate_weight = scatter_about(key_of[15], (EXPERT_COUNT, D, FFW), D ** -0.5, 0.078125, ((0, 8), (2, 32)))
    up_weight = scatter_about(key_of[16], (EXPERT_COUNT, D, FFW), D ** -0.5, 0.078125, ((0, 8), (2, 32)))
    down_projection_weight = scatter_about(key_of[17], (EXPERT_COUNT, FFW, D), FFW ** -0.5, 0.0625, ((0, 8), (1, 32)))
    return dict(hidden=hidden, queries=queries, new_keys=new_keys, new_values=new_values, cache_keys=cache_keys, cache_values=cache_values, lengths=lengths, page_table=page_table, resident=resident, prefix_keys=prefix_keys, prefix_values=prefix_values, out_weight=out_weight, norm_gain=norm_gain, router_weight=router_weight, experts=experts, gate_weight=gate_weight, up_weight=up_weight, down_projection_weight=down_projection_weight)


NEG = -1e+30
EPS = 1e-05

def holder_table(resident):
    flat = resident.reshape(-1)
    count = flat.shape[0]
    places = jnp.arange(count, dtype=jnp.int32)
    hits = flat[None, :] == jnp.arange(NPRE, dtype=jnp.int32)[:, None]
    return lax.optimization_barrier(jnp.min(jnp.where(hits, places[None, :], count), axis=1)).astype(jnp.int32)

def reference(hidden, queries, new_keys, new_values, cache_keys, cache_values, lengths, page_table, resident, prefix_keys, prefix_values, out_weight, norm_gain, router_weight, experts, gate_weight, up_weight, down_projection_weight):
    group = HQ // KVH
    scale = 1.0 / HD ** 0.5
    holder = holder_table(resident)
    pool_keys = prefix_keys.reshape(N_ROW * SLOTS, PAGE, KVH * HD)
    pool_values = prefix_values.reshape(N_ROW * SLOTS, PAGE, KVH * HD)
    page_rows = holder[page_table].astype(jnp.int32)

    def one_sequence(inputs):
        query, fresh_key, fresh_value, keys_own, values_own, length, rows_here = inputs
        keys = jnp.concatenate([pool_keys[rows_here].reshape(MAXP * PAGE, KVH, HD), keys_own.reshape(CTX, KVH, HD), fresh_key.reshape(1, KVH, HD)], axis=0).astype(jnp.float32)
        values = jnp.concatenate([pool_values[rows_here].reshape(MAXP * PAGE, KVH, HD), values_own.reshape(CTX, KVH, HD), fresh_value.reshape(1, KVH, HD)], axis=0).astype(jnp.float32)
        live = jnp.concatenate([jnp.ones((MAXP * PAGE,), jnp.bool_), jnp.arange(CTX, dtype=jnp.int32) < length, jnp.ones((1,), jnp.bool_)])
        scores = jnp.einsum('kgd,tkd->kgt', query.reshape(KVH, group, HD).astype(jnp.float32), keys) * scale
        scores = jnp.where(live[None, None, :], scores, NEG)
        peak = lax.optimization_barrier(jnp.max(scores, axis=-1, keepdims=True))
        expo = jnp.exp(scores - peak)
        total = lax.optimization_barrier(jnp.sum(expo, axis=-1, keepdims=True))
        weights = lax.optimization_barrier(expo.astype(jnp.bfloat16)).astype(jnp.float32)
        mixed = jnp.einsum('kgt,tkd->kgd', weights, values) / total
        return mixed.reshape(HQ * HD).astype(jnp.bfloat16)
    attended = lax.map(one_sequence, (queries, new_keys, new_values, cache_keys, cache_values, lengths, page_rows))
    projected = jnp.dot(attended, out_weight, preferred_element_type=jnp.float32)
    residual = hidden.astype(jnp.float32) + projected
    inverse = lax.rsqrt(lax.optimization_barrier(jnp.mean(residual * residual, axis=1)) + EPS)
    normed = (residual * inverse[:, None] * norm_gain[None, :]).astype(jnp.bfloat16)
    logits = jnp.dot(normed, router_weight, preferred_element_type=jnp.float32)
    chosen = jnp.take_along_axis(logits, experts, axis=1)
    first = 1.0 / (1.0 + jnp.exp(chosen[:, 1] - chosen[:, 0]))
    second = 1.0 / (1.0 + jnp.exp(chosen[:, 0] - chosen[:, 1]))
    hot = (experts[:, :, None] == jnp.arange(EXPERT_COUNT, dtype=jnp.int32)[None, None, :]).astype(jnp.int32)
    hot = hot.reshape(N_COL, TOK_COL * EXPERTS_PER_TOKEN, EXPERT_COUNT)
    ranks = lax.optimization_barrier(jnp.sum((jnp.cumsum(hot, axis=1) - hot) * hot, axis=2)).reshape(SEQS, EXPERTS_PER_TOKEN)
    blocks = (jnp.arange(SEQS, dtype=jnp.int32) // TOK_COL)[:, None]
    position = (blocks * CAP + ranks).astype(jnp.int32)
    owners = jnp.broadcast_to(jnp.arange(SEQS, dtype=jnp.int32)[:, None], (SEQS, EXPERTS_PER_TOKEN))
    rows_in = N_COL * CAP
    sources = jnp.full((EXPERT_COUNT, rows_in), SEQS, jnp.int32)
    sources = sources.at[experts.reshape(-1), position.reshape(-1)].set(owners.reshape(-1))
    padded = jnp.concatenate([normed, jnp.zeros((1, D), normed.dtype)], axis=0)

    def one_expert(inputs):
        source, gate_matrix, up_matrix, down_matrix = inputs
        taken = padded[source]
        inner_gate = jnp.dot(taken, gate_matrix, preferred_element_type=jnp.float32)
        inner_up = jnp.dot(taken, up_matrix, preferred_element_type=jnp.float32)
        activated_hidden = (jax.nn.silu(inner_gate) * inner_up).astype(jnp.bfloat16)
        return jnp.dot(activated_hidden, down_matrix, preferred_element_type=jnp.float32).astype(jnp.bfloat16)
    outputs = lax.map(one_expert, (sources, gate_weight, up_weight, down_projection_weight))
    first_out = outputs[experts[:, 0], position[:, 0]].astype(jnp.float32)
    second_out = outputs[experts[:, 1], position[:, 1]].astype(jnp.float32)
    return (residual + first[:, None] * first_out + second[:, None] * second_out).astype(jnp.bfloat16)
```

```python
import functools
import math

import jax
import jax.numpy as jnp
from jax import lax
from jax.experimental import pallas as pl
from jax.experimental.pallas import tpu as pltpu
from jax.sharding import PartitionSpec as P

D = 6144
HQ = 48
KVH = 8
HD = 128
GROUP = HQ // KVH
EXPERTS = 8
CAP = 4
NEG = -1e30
EPS = 1e-05
NX, NY, NCORE = 4, 4, 2
NR = NX * NY * NCORE
NC = 8
SEQS = 64
BLOCK = SEQS // NC
SLOTS = 4
PAGE = 128
KEYS = SLOTS * PAGE
CTX = 2048
WIDTH = D // NR
WPAD = 256
FSLICE = 256
ROWS = NC * CAP
HROWS = 16
SCALE = 1.0 / math.sqrt(HD)
F32 = jnp.float32
BF16 = jnp.bfloat16

ROW_PEERS = [
    (dx, dy, dc)
    for dx in range(NX)
    for dy in range(NY)
    for dc in range(NCORE)
    if (dx, dy, dc) != (0, 0, 0)
]
ROW_PEERS.sort(key=lambda t: -(min(t[0], NX - t[0]) + min(t[1], NY - t[1]) + 0.5 * t[2]))
COL_PEERS = sorted(range(1, NC), key=lambda d: -min(d, NC - d))


def iota(shape, dim):
    return lax.broadcasted_iota(jnp.int32, shape, dim)


def nt_dot(a, b):
    return lax.dot_general(a, b, (((1,), (1,)), ((), ())), preferred_element_type=F32)


def dot(a, b):
    return jnp.dot(a, b, preferred_element_type=F32)


def kernel(
    lengths,
    resident_s,
    experts_s,
    hidden,
    queries,
    new_keys,
    new_values,
    page_table,
    resident,
    gain,
    router,
    cache_keys,
    cache_values,
    prefix_keys,
    prefix_values,
    out_weight,
    gate_weight,
    up_weight,
    down_weight,
    out,
    kc,
    vc,
    pk,
    pv,
    wo,
    wg,
    wu,
    wd,
    qsend,
    qall,
    psend,
    prec,
    asend,
    aall,
    tsend,
    trec,
    xsend,
    xall,
    ysend,
    yrec,
    zsend,
    zrec,
    hsend,
    hrec,
    sel,
    cntk,
    disp,
    hot128,
    raug,
    gpad,
    hpad,
    pbs,
    hres,
    local_sem,
    send_sem,
    recv_sem,
):
    r = lax.axis_index("row")
    c = lax.axis_index("col")
    rx, ry, rc = r // (NY * NCORE), (r // NCORE) % NY, r % NCORE

    def row_peer(t):
        dx, dy, dc = t
        return ((rx + dx) % NX) * (NY * NCORE) + ((ry + dy) % NY) * NCORE + (rc + dc) % NCORE

    def col_peer(d):
        return (c + d) % NC

    barrier = pltpu.get_barrier_semaphore()
    for t in ROW_PEERS:
        pl.semaphore_signal(barrier, inc=1, device_id={"row": row_peer(t), "col": c}, device_id_type=pl.DeviceIdType.MESH)
    for d in COL_PEERS:
        pl.semaphore_signal(barrier, inc=1, device_id={"row": r, "col": col_peer(d)}, device_id_type=pl.DeviceIdType.MESH)

    loads = [
        pltpu.make_async_copy(s, t, local_sem.at[i])
        for i, (s, t) in enumerate(
            (
                (prefix_keys.at[0], pk),
                (prefix_values.at[0], pv),
                (cache_keys, kc),
                (cache_values, vc),
                (out_weight, wo),
                (gate_weight.at[0], wg),
                (up_weight.at[0], wu),
                (down_weight.at[0], wd),
            )
        )
    ]
    for load in loads:
        load.start()

    def to_row(phase, src_of, dst):
        for t in ROW_PEERS:
            peer = row_peer(t)
            pltpu.make_async_remote_copy(
                src_ref=src_of(peer),
                dst_ref=dst.at[r],
                send_sem=send_sem.at[phase],
                recv_sem=recv_sem.at[phase],
                device_id={"row": peer, "col": c},
                device_id_type=pl.DeviceIdType.MESH,
            ).start()

    def to_col(phase, src_of, dst):
        for d in COL_PEERS:
            peer = col_peer(d)
            pltpu.make_async_remote_copy(
                src_ref=src_of(peer),
                dst_ref=dst.at[c],
                send_sem=send_sem.at[phase],
                recv_sem=recv_sem.at[phase],
                device_id={"row": r, "col": peer},
                device_id_type=pl.DeviceIdType.MESH,
            ).start()

    def wait_for(sem, buffer, count):
        part = buffer.at[pl.ds(0, count)]
        pltpu.make_async_copy(part, part, sem).wait()

    q = queries[...].astype(F32)
    qrows = jnp.concatenate(
        [q[:, g * HD : (g + 1) * HD] for g in range(GROUP)] + [jnp.zeros((HROWS - 2 * GROUP, HD), F32)], axis=0
    )
    q16 = qrows.astype(BF16)
    qsend[...] = q16
    qall[r] = q16
    e_i, b_i = iota((EXPERTS, 128), 0), iota((EXPERTS, 128), 1)
    hot = jnp.zeros((EXPERTS, 128), F32)
    for b in range(BLOCK):
        named = (e_i == experts_s[b, 0]) | (e_i == experts_s[b, 1])
        hot = jnp.where(named & (b_i == c * BLOCK + b), 1.0, hot)
    hsend[...] = hot
    hrec[c] = hot

    pl.semaphore_wait(barrier, len(ROW_PEERS) + len(COL_PEERS))
    to_row(0, lambda peer: qsend, qall)
    to_col(1, lambda peer: hsend, hrec)

    lane64 = iota((SEQS, 128), 1)
    table = page_table[...]
    res = resident[...]
    flat = iota(res.shape, 0) * SLOTS + iota(res.shape, 1)
    for j in range(SLOTS):
        page = resident_s[r, j]
        earlier = jnp.sum(jnp.where((res == page) & (flat < r * SLOTS + j), 1.0, 0.0), keepdims=True)
        times = jnp.sum(jnp.where(table == page, 1.0, 0.0), axis=1, keepdims=True)
        times = jnp.where(earlier > 0.0, 0.0, times)
        cntk[:, j * PAGE : (j + 1) * PAGE] = jnp.broadcast_to(times, (SEQS, PAGE)).astype(BF16)
    for g in range(GROUP):
        want, have = iota((SEQS, NR * HROWS), 0), iota((SEQS, NR * HROWS), 1)
        there = (want // 2) * HROWS + 2 * g + want % 2
        sel[g * SEQS : (g + 1) * SEQS, :] = jnp.where(have == there, 1.0, 0.0).astype(BF16)
    place = jnp.where(
        (iota((EXPERTS, WPAD), 1) >= WIDTH) & (iota((EXPERTS, WPAD), 1) < WIDTH + 48)
        & ((iota((EXPERTS, WPAD), 1) - WIDTH) % 16 == iota((EXPERTS, WPAD), 0)), 1.0, 0.0
    ).astype(BF16)
    raug[...] = dot(router[...], place).astype(BF16)
    gpad[...] = jnp.zeros_like(gpad)
    gpad[0:1, 0:WIDTH] = gain[...]
    hpad[...] = jnp.zeros_like(hpad)
    hpad[:, 0:WIDTH] = hidden[...].astype(F32)
    pbs[...] = jnp.zeros_like(pbs)
    hot128[...] = jnp.zeros_like(hot128)

    loads[2].wait()
    odd = iota((HROWS, 1), 0) % 2 == 1
    own = [nt_dot(q16, kc[s]) for s in range(2)]
    scores = jnp.where(odd, own[1], own[0]) * SCALE
    length = jnp.where(odd, lengths[1], lengths[0])
    scores = jnp.where(iota((HROWS, CTX), 1) < length, scores, NEG)
    fresh_k = jnp.where(odd, new_keys[1:2, :].astype(F32), new_keys[0:1, :].astype(F32))
    fresh_v = jnp.where(odd, new_values[1:2, :].astype(F32), new_values[0:1, :].astype(F32))
    fresh = jnp.sum(qrows * fresh_k, axis=1, keepdims=True) * SCALE
    peak = jnp.maximum(jnp.max(scores, axis=1, keepdims=True), fresh)
    expo = jnp.exp(scores - peak)
    fresh_e = jnp.exp(fresh - peak)
    own_total = jnp.sum(expo, axis=1, keepdims=True) + fresh_e
    loads[3].wait()
    mixed = (
        dot(jnp.where(odd, 0.0, expo).astype(BF16), vc[0])
        + dot(jnp.where(odd, expo, 0.0).astype(BF16), vc[1])
        + fresh_e.astype(BF16).astype(F32) * fresh_v
    )
    own_peak = peak

    loads[0].wait()
    loads[1].wait()
    wait_for(recv_sem.at[0], qall, NR - 1)
    CH = 8
    for i in range(NR // CH):
        n = CH * HROWS
        qs = qall[i * CH : (i + 1) * CH].reshape(n, HD)
        row = iota((n, SEQS), 0)
        member = (i * CH + row // HROWS) * 2 + row % 2 == iota((n, SEQS), 1)
        times = dot(jnp.where(member, 1.0, 0.0).astype(BF16), cntk[...])
        s = nt_dot(qs, pk[...].reshape(KEYS, HD)) * SCALE
        s = jnp.where(times > 0.0, s, NEG)
        m = jnp.max(s, axis=1, keepdims=True)
        e = jnp.exp(s - m) * times
        l = jnp.sum(e, axis=1, keepdims=True)
        o = dot(e.astype(BF16), pv[...].reshape(KEYS, HD))
        some = l > 0.0
        safe = jnp.where(some, l, 1.0)
        o = o / safe
        lse = jnp.where(some, m + jnp.log(safe), NEG)
        k_i = iota((n, HD), 0) % HROWS
        diag = jnp.where(k_i == iota((n, HD), 1), lse, 0.0)
        across = jnp.sum(diag.reshape(CH, HROWS, HD), axis=1, keepdims=True)
        across = jnp.broadcast_to(across, (CH, HROWS, HD)).reshape(n, HD)
        hi = across.astype(BF16).astype(F32)
        mid = (across - hi).astype(BF16).astype(F32)
        lo = across - hi - mid
        tail = jnp.where(k_i == 12, hi, jnp.where(k_i == 13, mid, jnp.where(k_i == 14, lo, 0.0)))
        psend[i * CH : (i + 1) * CH] = jnp.where(k_i < 12, o, tail).astype(BF16).reshape(CH, HROWS, HD)
    prec[r] = psend[r]
    to_row(2, lambda peer: psend.at[peer], prec)

    wait_for(recv_sem.at[1], hrec, NC - 1)
    hot = jnp.sum(hrec[...], axis=0)
    hot128[0:EXPERTS, :] = hot
    u0, u1 = iota((128, 128), 0), iota((128, 128), 1)
    before = jnp.where((u0 < u1) & (u0 // BLOCK == u1 // BLOCK), 1.0, 0.0).astype(BF16)
    rank = dot(hot.astype(BF16), before)
    d_r, d_l = iota((ROWS, 128), 0), iota((ROWS, 128), 1)
    for e in range(EXPERTS):
        hit = (
            (hot[e : e + 1, :] > 0.0)
            & (rank[e : e + 1, :] == (d_r % CAP).astype(F32))
            & (d_l // BLOCK == d_r // CAP)
        )
        home = d_l % SEQS == e * BLOCK + d_r % BLOCK
        low = jnp.where(hit & (d_l < SEQS), 1.0, 0.0) + jnp.where(
            home & (d_l >= SEQS) & (d_r // BLOCK == 0), 1.0, 0.0
        )
        high = jnp.where(home & (d_r // BLOCK == 1 + d_l // SEQS), 1.0, 0.0)
        disp[e * ROWS : (e + 1) * ROWS, 0:128] = low.astype(BF16)
        disp[e * ROWS : (e + 1) * ROWS, 128:256] = high.astype(BF16)

    wait_for(recv_sem.at[2], prec, NR - 1)
    parts = prec[...].astype(F32)
    lrow = parts[:, 12:13, :] + parts[:, 13:14, :] + parts[:, 14:15, :]
    on_diag = iota((NR, HROWS, HD), 1) == iota((NR, HROWS, HD), 2)
    lse = jnp.sum(jnp.where(on_diag, jnp.broadcast_to(lrow, (NR, HROWS, HD)), 0.0), axis=2, keepdims=True)
    lse = jnp.where(iota((NR, HROWS, 1), 1) < 12, lse, NEG)
    top = jnp.maximum(jnp.max(lse, axis=0), own_peak)
    w = jnp.exp(lse - top[None])
    w_own = jnp.exp(own_peak - top)
    total = jnp.sum(w, axis=0) + own_total * w_own
    mixed = jnp.sum(w * parts, axis=0) + mixed * w_own
    att = jnp.where(iota((HROWS, HD), 0) < 12, mixed / total, 0.0).astype(BF16)
    asend[...] = att
    aall[r] = att
    to_row(3, lambda peer: asend, aall)

    loads[4].wait()
    wait_for(recv_sem.at[3], aall, NR - 1)
    picked = dot(sel[...], aall[...].reshape(NR * HROWS, HD)).astype(BF16)
    projected = dot(picked[0:SEQS], wo[0:HD, :])
    for g in range(1, GROUP):
        projected = projected + dot(picked[g * SEQS : (g + 1) * SEQS], wo[g * HD : (g + 1) * HD, :])
    pbs[:, 0:WIDTH] = projected
    plain = pbs[...]
    here = jnp.where(iota((SEQS, BLOCK), 0) == c * BLOCK + iota((SEQS, BLOCK), 1), 1.0, 0.0).astype(BF16)
    with_hidden = plain + dot(here, hpad[...].astype(BF16))
    lane = iota((SEQS, WPAD), 1)
    moved = [jnp.where(lane >= WIDTH, pltpu.roll(plain, WIDTH - 64 * i, 1), 0.0) for i in range(3)]
    stacked = jnp.concatenate([with_hidden] + moved, axis=0).astype(BF16)
    tsend[...] = dot(disp[...], stacked).astype(BF16).reshape(NC, ROWS, WPAD)
    trec[c] = tsend[c]
    to_col(4, lambda peer: tsend.at[peer], trec)

    wait_for(recv_sem.at[4], trec, NC - 1)
    resid = jnp.sum(trec[...].astype(F32), axis=0)
    lane8 = iota((BLOCK, WPAD), 1)
    home = hpad[...]
    for i in range(3):
        piece = pltpu.roll(resid[i * BLOCK : (i + 1) * BLOCK, :], (64 * i + 64) % WPAD, 1)
        home = home + jnp.where(lane8 // 64 == i, piece, 0.0)
    hres[...] = home
    lane32 = iota((ROWS, WPAD), 1)
    squares = jnp.sum(jnp.where(lane32 < WIDTH, resid * resid, 0.0), axis=1, keepdims=True)
    x = resid * gpad[0:1, :]
    stats = dot(x[:, 0:WIDTH].astype(BF16), raug[...])
    stats = stats + jnp.where((lane32 >= WIDTH) & ((lane32 - WIDTH) % 16 == 8), squares, 0.0)
    hi = stats.astype(BF16).astype(F32)
    mid = (stats - hi).astype(BF16).astype(F32)
    lo = stats - hi - mid
    x = jnp.where(lane32 < WIDTH, x, jnp.where(lane32 < WIDTH + 16, hi, jnp.where(lane32 < WIDTH + 32, mid, jnp.where(lane32 < WIDTH + 48, lo, 0.0))))
    x = x.astype(BF16)
    xsend[...] = x
    xall[r] = x
    to_row(5, lambda peer: xsend, xall)

    loads[5].wait()
    loads[6].wait()
    mine = disp[pl.ds(pl.multiple_of(c * ROWS, ROWS), ROWS), 0:128]
    mine = jnp.where(iota((ROWS, 128), 1) < SEQS, mine.astype(F32), 0.0)
    wait_for(recv_sem.at[5], xall, NR - 1)

    def expert_step(i, carry):
        g, u, st = carry
        xi = xall[i]
        rows = pl.ds(pl.multiple_of(i * WIDTH, 64), WIDTH)
        g = g + dot(xi[:, 0:WIDTH], wg[rows, :])
        u = u + dot(xi[:, 0:WIDTH], wu[rows, :])
        st = st + xi[:, 128:256].astype(F32)
        return g, u, st

    inner_gate, inner_up, st = lax.fori_loop(
        0, NR, expert_step,
        (jnp.zeros((ROWS, FSLICE), F32), jnp.zeros((ROWS, FSLICE), F32), jnp.zeros((ROWS, 128), F32)),
    )
    st = st + pltpu.roll(st, 112, 1) + pltpu.roll(st, 96, 1)
    st = pltpu.roll(st, 64, 1)
    lane128 = iota((ROWS, 128), 1)
    squares = jnp.sum(jnp.where(lane128 == 8, st, 0.0), axis=1, keepdims=True)
    inverse = lax.rsqrt(squares / D + EPS)
    pair = nt_dot(mine.astype(BF16), hot128[...].astype(BF16))
    logits = st * inverse
    own_logit = jnp.sum(jnp.where(lane128 == c, logits, 0.0), axis=1, keepdims=True)
    other = jnp.sum(jnp.where((pair > 0.0) & (lane128 != c), logits, 0.0), axis=1, keepdims=True)
    share = 1.0 / (1.0 + jnp.exp(other - own_logit))
    inner_gate = inner_gate * inverse
    inner_up = inner_up * inverse
    act = (inner_gate / (1.0 + jnp.exp(-inner_gate)) * inner_up * share).astype(BF16)
    loads[7].wait()
    for k in range(NR // 2):
        y = dot(act, wd[:, k * 2 * WIDTH : (k + 1) * 2 * WIDTH])
        ysend[2 * k] = y[:, 0:WPAD].astype(BF16)
        ysend[2 * k + 1] = pltpu.roll(y[:, 128 : 128 + WPAD], WPAD - 64, 1).astype(BF16)
    yrec[r] = ysend[r]
    to_row(6, lambda peer: ysend.at[peer], yrec)

    wait_for(recv_sem.at[6], yrec, NR - 1)
    ysum = lax.fori_loop(0, NR, lambda i, acc: acc + yrec[i].astype(F32), jnp.zeros((ROWS, WPAD), F32))
    back = lax.dot_general(
        mine.astype(BF16), ysum.astype(BF16), (((0,), (0,)), ((), ())), preferred_element_type=F32
    )
    for i in range(NC):
        both = jnp.concatenate(
            [back[i * BLOCK : (i + 1) * BLOCK, 0:128], back[i * BLOCK : (i + 1) * BLOCK, 128:256]], axis=0
        )
        zsend[i] = both.astype(BF16)
    zrec[c] = zsend[c]
    to_col(7, lambda peer: zsend.at[peer], zrec)
    wait_for(recv_sem.at[7], zrec, NC - 1)
    z = jnp.sum(zrec[...].astype(F32), axis=0)
    final = hres[...]
    out[:, 0:128] = (final[:, 0:128] + z[0:BLOCK]).astype(out.dtype)
    out[:, 128:WIDTH] = (final[:, 128:WIDTH] + z[BLOCK:, 0 : WIDTH - 128]).astype(out.dtype)

    wait_for(send_sem.at[0], qall, NR - 1)
    wait_for(send_sem.at[1], hrec, NC - 1)
    wait_for(send_sem.at[2], prec, NR - 1)
    wait_for(send_sem.at[3], aall, NR - 1)
    wait_for(send_sem.at[4], trec, NC - 1)
    wait_for(send_sem.at[5], xall, NR - 1)
    wait_for(send_sem.at[6], yrec, NR - 1)
    wait_for(send_sem.at[7], zrec, NC - 1)


def body(
    hidden,
    queries,
    new_keys,
    new_values,
    cache_keys,
    cache_values,
    lengths,
    page_table,
    resident,
    prefix_keys,
    prefix_values,
    out_weight,
    norm_gain,
    router_weight,
    experts,
    gate_weight,
    up_weight,
    down_projection_weight,
):
    smem = pl.BlockSpec(memory_space=pltpu.SMEM)
    vmem = pl.BlockSpec(memory_space=pltpu.VMEM)
    anyw = pl.BlockSpec(memory_space=pl.ANY)
    return pl.pallas_call(
        kernel,
        out_shape=jax.ShapeDtypeStruct((BLOCK, WIDTH), BF16),
        in_specs=[smem] * 3 + [vmem] * 8 + [anyw] * 8,
        out_specs=vmem,
        scratch_shapes=[
            pltpu.VMEM((2, CTX, HD), BF16),
            pltpu.VMEM((2, CTX, HD), BF16),
            pltpu.VMEM((SLOTS, PAGE, HD), BF16),
            pltpu.VMEM((SLOTS, PAGE, HD), BF16),
            pltpu.VMEM((GROUP * HD, WIDTH), BF16),
            pltpu.VMEM((D, FSLICE), BF16),
            pltpu.VMEM((D, FSLICE), BF16),
            pltpu.VMEM((FSLICE, D), BF16),
            pltpu.VMEM((HROWS, HD), BF16),
            pltpu.VMEM((NR, HROWS, HD), BF16),
            pltpu.VMEM((NR, HROWS, HD), BF16),
            pltpu.VMEM((NR, HROWS, HD), BF16),
            pltpu.VMEM((HROWS, HD), BF16),
            pltpu.VMEM((NR, HROWS, HD), BF16),
            pltpu.VMEM((NC, ROWS, WPAD), BF16),
            pltpu.VMEM((NC, ROWS, WPAD), BF16),
            pltpu.VMEM((ROWS, WPAD), BF16),
            pltpu.VMEM((NR, ROWS, WPAD), BF16),
            pltpu.VMEM((NR, ROWS, WPAD), BF16),
            pltpu.VMEM((NR, ROWS, WPAD), BF16),
            pltpu.VMEM((NC, 2 * BLOCK, 128), BF16),
            pltpu.VMEM((NC, 2 * BLOCK, 128), BF16),
            pltpu.VMEM((EXPERTS, 128), F32),
            pltpu.VMEM((NC, EXPERTS, 128), F32),
            pltpu.VMEM((GROUP * SEQS, NR * HROWS), BF16),
            pltpu.VMEM((SEQS, KEYS), BF16),
            pltpu.VMEM((NC * ROWS, WPAD), BF16),
            pltpu.VMEM((128, 128), F32),
            pltpu.VMEM((WIDTH, WPAD), BF16),
            pltpu.VMEM((8, WPAD), F32),
            pltpu.VMEM((BLOCK, WPAD), F32),
            pltpu.VMEM((SEQS, WPAD), F32),
            pltpu.VMEM((BLOCK, WPAD), F32),
            pltpu.SemaphoreType.DMA((8,)),
            pltpu.SemaphoreType.DMA((8,)),
            pltpu.SemaphoreType.DMA((8,)),
        ],
        compiler_params=pltpu.CompilerParams(
            collective_id=0, has_side_effects=True, vmem_limit_bytes=48 * 1024 * 1024
        ),
        name="layer",
    )(
        lengths,
        resident,
        experts,
        hidden,
        queries,
        new_keys,
        new_values,
        page_table,
        resident,
        norm_gain.reshape(1, WIDTH),
        router_weight,
        cache_keys,
        cache_values,
        prefix_keys,
        prefix_values,
        out_weight,
        gate_weight,
        up_weight,
        down_projection_weight,
    )


def solution(mesh):
    in_specs = (
        P("col", "row"),
        P("row", "col"),
        P("row", "col"),
        P("row", "col"),
        P("row", None, "col"),
        P("row", None, "col"),
        P("row"),
        P(),
        P(),
        P("row", None, None, "col"),
        P("row", None, None, "col"),
        P("col", "row"),
        P("row"),
        P("row", None),
        P("col", None),
        P("col", None, "row"),
        P("col", None, "row"),
        P("col", "row", None),
    )
    return jax.shard_map(body, mesh=mesh, in_specs=in_specs, out_specs=P("col", "row"), check_vma=False)
```

```python
import functools
import math

import jax
import jax.numpy as jnp
from jax import lax
from jax.experimental import pallas as pl
from jax.experimental.pallas import tpu as pltpu
from jax.sharding import PartitionSpec as P

D = 6144
HQ = 48
KVH = 8
HD = 128
GROUP = HQ // KVH
EXPERTS = 8
CAP = 4
NEG = -1e30
EPS = 1e-05
NX, NY, NCORE = 4, 4, 2
NR = NX * NY * NCORE
NC = 8
SEQS = 64
BLOCK = SEQS // NC
SLOTS = 4
PAGE = 128
KEYS = SLOTS * PAGE
CTX = 2048
WIDTH = D // NR
WPAD = 256
FSLICE = 256
ROWS = NC * CAP
HROWS = 16
SCALE = 1.0 / math.sqrt(HD)
F32 = jnp.float32
BF16 = jnp.bfloat16

ROW_PEERS = [
    (dx, dy, dc)
    for dx in range(NX)
    for dy in range(NY)
    for dc in range(NCORE)
    if (dx, dy, dc) != (0, 0, 0)
]
ROW_PEERS.sort(key=lambda t: -(min(t[0], NX - t[0]) + min(t[1], NY - t[1]) + 0.5 * t[2]))
PER_X = NY * NCORE
NEAR_FIRST = (0, 1, 3, 2)
ARRIVAL = (2, 1, 3, 0)
ORDER1 = (0, 1, 3, 2)
ORDER2 = (0, 1, 3, 2)
ORDER3 = (2, 1, 3, 0)
FAR_FIRST = (2, 1, 3, 0)
CHIP_PEERS = [t for t in ROW_PEERS if t[2] == 0]
CHIPS = NX * NY
COL_PEERS = sorted(range(1, NC), key=lambda d: -min(d, NC - d))


def iota(shape, dim):
    return lax.broadcasted_iota(jnp.int32, shape, dim)


def nt_dot(a, b):
    return lax.dot_general(a, b, (((1,), (1,)), ((), ())), preferred_element_type=F32)


def dot(a, b):
    return jnp.dot(a, b, preferred_element_type=F32)


def kernel(
    lengths_h,
    resident_h,
    experts_h,
    hidden_h,
    queries_h,
    new_keys_h,
    new_values_h,
    page_table_h,
    gain_h,
    router_h,
    cache_keys,
    cache_values,
    prefix_keys,
    prefix_values,
    out_weight,
    gate_weight,
    up_weight,
    down_weight,
    out,
    lengths,
    resident_s,
    experts_s,
    hidden,
    queries,
    new_keys,
    new_values,
    page_table,
    resident,
    gain,
    router,
    kc,
    vc,
    pk,
    pv,
    wo,
    wg,
    wu,
    wd,
    qsend,
    qall,
    psend,
    prec,
    asend,
    aall,
    tsend,
    trec,
    xsend,
    xall,
    asend2,
    arecv2,
    ypair,
    yrec,
    zsend,
    zrec,
    hsend,
    hrec,
    sel,
    cntk,
    disp,
    hot128,
    raug,
    gpad,
    hpad,
    hplaced,
    pbs,
    attended,
    hres,
    local_sem,
    down_sem,
    send_sem,
    recv_sem,
):
    r = lax.axis_index("row")
    c = lax.axis_index("col")
    rx, ry, rc = r // (NY * NCORE), (r // NCORE) % NY, r % NCORE

    def row_peer(t):
        dx, dy, dc = t
        return ((rx + dx) % NX) * (NY * NCORE) + ((ry + dy) % NY) * NCORE + (rc + dc) % NCORE

    def col_peer(d):
        return (c + d) % NC

    barrier = pltpu.get_barrier_semaphore()
    for t in ROW_PEERS:
        pl.semaphore_signal(barrier, inc=1, device_id={"row": row_peer(t), "col": c}, device_id_type=pl.DeviceIdType.MESH)
    for d in COL_PEERS:
        pl.semaphore_signal(barrier, inc=1, device_id={"row": r, "col": col_peer(d)}, device_id_type=pl.DeviceIdType.MESH)

    loads = [
        pltpu.make_async_copy(s, t, local_sem.at[i])
        for i, (s, t) in enumerate(
            (
                (queries_h, queries),
                (experts_h, experts_s),
                (cache_keys, kc),
                (cache_values, vc),
                (prefix_keys.at[0], pk),
                (prefix_values.at[0], pv),
                (lengths_h, lengths),
                (new_keys_h, new_keys),
                (new_values_h, new_values),
                (resident_h, resident_s),
                (resident_h, resident),
                (page_table_h, page_table),
                (router_h, router),
                (gain_h, gain),
                (hidden_h, hidden),
                (out_weight, wo),
                (gate_weight.at[0], wg),
                (up_weight.at[0], wu),
            )
        )
    ]
    loads += [
        pltpu.make_async_copy(
            down_weight.at[0, :, pl.ds(pl.multiple_of(2 * WIDTH * k + 128 * rc, 128), WPAD)],
            wd.at[k, pl.ds(pl.multiple_of(rc * FSLICE, FSLICE), FSLICE)],
            down_sem.at[0],
        )
        for k in range(CHIPS)
    ]
    for load in loads:
        load.start()

    def to_row(phase, src_of, dst, only=None):
        for t in ROW_PEERS:
            if only is not None and t[0] != only:
                continue
            peer = row_peer(t)
            pltpu.make_async_remote_copy(
                src_ref=src_of(peer),
                dst_ref=dst.at[r],
                send_sem=send_sem.at[phase],
                recv_sem=recv_sem.at[phase, (NX - t[0]) % NX],
                device_id={"row": peer, "col": c},
                device_id_type=pl.DeviceIdType.MESH,
            ).start()

    def to_chips(phase, src_of, dst, only=None):
        for t in CHIP_PEERS:
            if only is not None and t[0] != only:
                continue
            peer = row_peer(t)
            pltpu.make_async_remote_copy(
                src_ref=src_of(peer // NCORE),
                dst_ref=dst,
                send_sem=send_sem.at[phase],
                recv_sem=recv_sem.at[phase, (NX - t[0]) % NX],
                device_id={"row": peer, "col": c},
                device_id_type=pl.DeviceIdType.MESH,
            ).start()

    def to_partner(phase, src, dst, dx):
        pltpu.make_async_remote_copy(
            src_ref=src,
            dst_ref=dst,
            send_sem=send_sem.at[phase],
            recv_sem=recv_sem.at[phase, dx],
            device_id={"row": row_peer((0, 0, 1)), "col": c},
            device_id_type=pl.DeviceIdType.MESH,
        ).start()

    def chips_of(dx):
        return pl.ds(((rx + dx) % NX) * NY, NY)

    def to_col(phase, src_of, dst):
        for d in COL_PEERS:
            peer = col_peer(d)
            pltpu.make_async_remote_copy(
                src_ref=src_of(peer),
                dst_ref=dst.at[c],
                send_sem=send_sem.at[phase],
                recv_sem=recv_sem.at[phase, 0],
                device_id={"row": r, "col": peer},
                device_id_type=pl.DeviceIdType.MESH,
            ).start()

    def wait_for(sem, buffer, count):
        part = buffer.at[pl.ds(0, count)]
        pltpu.make_async_copy(part, part, sem).wait()

    def first_of(dx):
        return ((rx + dx) % NX) * PER_X

    def group_here(phase, buffer, dx):
        wait_for(recv_sem.at[phase, dx], buffer, PER_X - 1 if dx == 0 else PER_X)

    loads[0].wait()
    loads[1].wait()
    q = queries[...].astype(F32)
    qrows = jnp.concatenate(
        [q[:, g * HD : (g + 1) * HD] for g in range(GROUP)] + [jnp.zeros((HROWS - 2 * GROUP, HD), F32)], axis=0
    )
    q16 = qrows.astype(BF16)
    qsend[...] = q16
    qall[r] = q16
    e_i, b_i = iota((EXPERTS, 128), 0), iota((EXPERTS, 128), 1)
    hot = jnp.zeros((EXPERTS, 128), F32)
    for b in range(BLOCK):
        named = (e_i == experts_s[0, b]) | (e_i == experts_s[1, b])
        hot = jnp.where(named & (b_i == c * BLOCK + b), 1.0, hot)
    hsend[...] = hot
    hrec[c] = hot

    pl.semaphore_wait(barrier, len(ROW_PEERS) + len(COL_PEERS))
    to_row(0, lambda peer: qsend, qall)
    to_col(1, lambda peer: hsend, hrec)

    for k in range(CHIPS):
        pltpu.make_async_remote_copy(
            src_ref=down_weight.at[0, :, pl.ds(pl.multiple_of(2 * WIDTH * k + 128 * (1 - rc), 128), WPAD)],
            dst_ref=wd.at[k, pl.ds(pl.multiple_of(rc * FSLICE, FSLICE), FSLICE)],
            send_sem=down_sem.at[1],
            recv_sem=down_sem.at[2],
            device_id={"row": row_peer((0, 0, 1)), "col": c},
            device_id_type=pl.DeviceIdType.MESH,
        ).start()

    for i in range(9, 15):
        loads[i].wait()
    table = page_table[...]
    res = resident[...]
    flat = iota(res.shape, 1) * SLOTS + iota(res.shape, 0)
    for j in range(SLOTS):
        page = resident_s[j, r]
        earlier = jnp.sum(jnp.where((res == page) & (flat < r * SLOTS + j), 1.0, 0.0), keepdims=True)
        times = jnp.where((table == page) & (earlier == 0.0), 1.0, 0.0)
        cntk[j * PAGE : (j + 1) * PAGE, :] = jnp.broadcast_to(jnp.sum(times, axis=0, keepdims=True), (PAGE, SEQS)).astype(BF16)
    want, have = iota((GROUP * 2 * PER_X, PER_X * HROWS), 0), iota((GROUP * 2 * PER_X, PER_X * HROWS), 1)
    token = want % (2 * PER_X)
    there = (token // 2) * HROWS + 2 * (want // (2 * PER_X)) + token % 2
    sel[...] = jnp.where(have == there, 1.0, 0.0).astype(BF16)
    here = jnp.where(iota((SEQS, BLOCK), 0) == c * BLOCK + iota((SEQS, BLOCK), 1), 1.0, 0.0).astype(BF16)
    place = jnp.where(
        (iota((EXPERTS, WPAD), 1) >= WIDTH) & (iota((EXPERTS, WPAD), 1) < WIDTH + 48)
        & ((iota((EXPERTS, WPAD), 1) - WIDTH) % 16 == iota((EXPERTS, WPAD), 0)), 1.0, 0.0
    ).astype(BF16)
    raug[...] = lax.dot_general(router[...], place, (((0,), (0,)), ((), ())), preferred_element_type=F32).astype(BF16)
    gpad[...] = jnp.zeros_like(gpad)
    gpad[0:1, 0:WIDTH] = gain[...]
    hpad[...] = jnp.zeros_like(hpad)
    hpad[:, 0:WIDTH] = hidden[...].astype(F32)
    hplaced[...] = dot(here, hpad[...].astype(BF16))
    pbs[...] = jnp.zeros_like(pbs)
    hot128[...] = jnp.zeros_like(hot128)

    for i in (2, 6, 7, 8):
        loads[i].wait()
    odd = iota((HROWS, 1), 0) % 2 == 1
    own = [nt_dot(q16, kc[s]) for s in range(2)]
    scores = jnp.where(odd, own[1], own[0]) * SCALE
    length = jnp.where(odd, lengths[1], lengths[0])
    scores = jnp.where(iota((HROWS, CTX), 1) < length, scores, NEG)
    fresh_k = jnp.where(odd, new_keys[1:2, :].astype(F32), new_keys[0:1, :].astype(F32))
    fresh_v = jnp.where(odd, new_values[1:2, :].astype(F32), new_values[0:1, :].astype(F32))
    fresh = jnp.sum(qrows * fresh_k, axis=1, keepdims=True) * SCALE
    peak = jnp.maximum(jnp.max(scores, axis=1, keepdims=True), fresh)
    expo = jnp.exp(scores - peak)
    fresh_e = jnp.exp(fresh - peak)
    own_total = jnp.sum(expo, axis=1, keepdims=True) + fresh_e
    loads[3].wait()
    mixed = (
        dot(jnp.where(odd, 0.0, expo).astype(BF16), vc[0])
        + dot(jnp.where(odd, expo, 0.0).astype(BF16), vc[1])
        + fresh_e.astype(BF16).astype(F32) * fresh_v
    )
    own_peak = peak

    loads[4].wait()
    loads[5].wait()
    n = PER_X * HROWS
    k_i = iota((n, HD), 0) % HROWS
    seq = (iota((n, SEQS), 0) // HROWS) * 2 + iota((n, SEQS), 0) % 2
    for dx in ORDER1:
        group_here(0, qall, dx)
        base = first_of(dx)
        qs = qall[pl.ds(base, PER_X)].reshape(n, HD)
        member = seq + 2 * base == iota((n, SEQS), 1)
        times = nt_dot(jnp.where(member, 1.0, 0.0).astype(BF16), cntk[...])
        sc = nt_dot(qs, pk[...].reshape(KEYS, HD)) * SCALE
        sc = jnp.where(times > 0.0, sc, NEG)
        m = jnp.max(sc, axis=1, keepdims=True)
        e = jnp.exp(sc - m) * times
        l = jnp.sum(e, axis=1, keepdims=True)
        o = dot(e.astype(BF16), pv[...].reshape(KEYS, HD))
        some = l > 0.0
        safe = jnp.where(some, l, 1.0)
        o = o / safe
        lse = jnp.where(some, m + jnp.log(safe), NEG)
        diag = jnp.where(k_i == iota((n, HD), 1), lse, 0.0)
        across = jnp.sum(diag.reshape(PER_X, HROWS, HD), axis=1, keepdims=True)
        across = jnp.broadcast_to(across, (PER_X, HROWS, HD)).reshape(n, HD)
        hi = across.astype(BF16).astype(F32)
        mid = (across - hi).astype(BF16).astype(F32)
        lo = across - hi - mid
        tail = jnp.where(k_i == 12, hi, jnp.where(k_i == 13, mid, jnp.where(k_i == 14, lo, 0.0)))
        psend[pl.ds(base, PER_X)] = jnp.where(k_i < 12, o, tail).astype(BF16).reshape(PER_X, HROWS, HD)
        if dx == 0:
            prec[r] = psend[r]
        to_row(2, lambda peer: psend.at[peer], prec, dx)

    wait_for(recv_sem.at[1, 0], hrec, NC - 1)
    hot = jnp.sum(hrec[...], axis=0)
    hot128[0:EXPERTS, :] = hot
    u0, u1 = iota((128, 128), 0), iota((128, 128), 1)
    before = jnp.where((u0 < u1) & (u0 // BLOCK == u1 // BLOCK), 1.0, 0.0).astype(BF16)
    rank = dot(hot.astype(BF16), before)
    d_r, d_l = iota((ROWS, 128), 0), iota((ROWS, 128), 1)
    for e in range(EXPERTS):
        hit = (
            (hot[e : e + 1, :] > 0.0)
            & (rank[e : e + 1, :] == (d_r % CAP).astype(F32))
            & (d_l // BLOCK == d_r // CAP)
        )
        home = d_l % SEQS == e * BLOCK + d_r % BLOCK
        low = jnp.where(hit & (d_l < SEQS), 1.0, 0.0) + jnp.where(
            home & (d_l >= SEQS) & (d_r // BLOCK == 0), 1.0, 0.0
        )
        high = jnp.where(home & (d_r // BLOCK == 1 + d_l // SEQS), 1.0, 0.0)
        disp[e * ROWS : (e + 1) * ROWS, 0:128] = low.astype(BF16)
        disp[e * ROWS : (e + 1) * ROWS, 128:256] = high.astype(BF16)

    on_diag = iota((PER_X, HROWS, HD), 1) == iota((PER_X, HROWS, HD), 2)
    real = iota((PER_X, HROWS, 1), 1) < 12
    merged = [(own_peak, own_total, mixed)]
    for dx in ORDER2:
        group_here(2, prec, dx)
        parts = prec[pl.ds(first_of(dx), PER_X)].astype(F32)
        lrow = parts[:, 12:13, :] + parts[:, 13:14, :] + parts[:, 14:15, :]
        lse = jnp.sum(jnp.where(on_diag, jnp.broadcast_to(lrow, parts.shape), 0.0), axis=2, keepdims=True)
        lse = jnp.where(real, lse, NEG)
        top = jnp.max(lse, axis=0)
        w = jnp.exp(lse - top[None])
        w = jnp.where(lse > 0.5 * NEG, w, 0.0)
        merged.append((top, jnp.sum(w, axis=0), jnp.sum(w * parts, axis=0)))
    top = functools.reduce(jnp.maximum, [m for m, _, _ in merged])
    ws = [jnp.exp(m - top) for m, _, _ in merged]
    total = sum(w * l for w, (_, l, _) in zip(ws, merged))
    mixed = sum(w * o for w, (_, _, o) in zip(ws, merged))
    att = jnp.where(iota((HROWS, HD), 0) < 12, mixed / total, 0.0).astype(BF16)
    asend[...] = att
    aall[r] = att
    to_row(3, lambda peer: asend, aall)

    loads[15].wait()
    for dx in ORDER3:
        group_here(3, aall, dx)
        base = first_of(dx)
        picked = dot(sel[...], aall[pl.ds(base, PER_X)].reshape(PER_X * HROWS, HD)).astype(BF16)
        tokens = 2 * PER_X
        heads = jnp.concatenate([picked[g * tokens : (g + 1) * tokens] for g in range(GROUP)], axis=1)
        attended[pl.ds(pl.multiple_of(2 * base, tokens), tokens), :] = heads
    pbs[:, 0:WIDTH] = nt_dot(attended[...], wo[...])
    plain = pbs[...]
    with_hidden = plain + hplaced[...]
    lane = iota((SEQS, WPAD), 1)
    moved = [jnp.where(lane >= WIDTH, pltpu.roll(plain, WIDTH - 64 * i, 1), 0.0) for i in range(3)]
    stacked = jnp.concatenate([with_hidden] + moved, axis=0).astype(BF16)
    tsend[...] = dot(disp[...], stacked).astype(BF16).reshape(NC, ROWS, WPAD)
    trec[c] = tsend[c]
    to_col(4, lambda peer: tsend.at[peer], trec)

    wait_for(recv_sem.at[4, 0], trec, NC - 1)
    resid = jnp.sum(trec[...].astype(F32), axis=0)
    lane8 = iota((BLOCK, WPAD), 1)
    home = hpad[...]
    for i in range(3):
        piece = pltpu.roll(resid[i * BLOCK : (i + 1) * BLOCK, :], (64 * i + 64) % WPAD, 1)
        home = home + jnp.where(lane8 // 64 == i, piece, 0.0)
    hres[...] = home
    lane32 = iota((ROWS, WPAD), 1)
    squares = jnp.sum(jnp.where(lane32 < WIDTH, resid * resid, 0.0), axis=1, keepdims=True)
    x = resid * gpad[0:1, :]
    stats = dot(x[:, 0:WIDTH].astype(BF16), raug[...])
    stats = stats + jnp.where((lane32 >= WIDTH) & ((lane32 - WIDTH) % 16 == 8), squares, 0.0)
    hi = stats.astype(BF16).astype(F32)
    mid = (stats - hi).astype(BF16).astype(F32)
    lo = stats - hi - mid
    x = jnp.where(lane32 < WIDTH, x, jnp.where(lane32 < WIDTH + 16, hi, jnp.where(lane32 < WIDTH + 32, mid, jnp.where(lane32 < WIDTH + 48, lo, 0.0))))
    x = jnp.where(rc == 0, x, pltpu.roll(x, 64, 1)).astype(BF16)
    xsend[...] = x
    chip = r // NCORE
    xall[rc, chip] = x
    to_chips(5, lambda peer: xsend, xall.at[rc, chip])

    loads[16].wait()
    loads[17].wait()
    mine = disp[pl.ds(pl.multiple_of(c * ROWS, ROWS), ROWS), 0:128]
    mine = jnp.where(iota((ROWS, 128), 1) < SEQS, mine.astype(F32), 0.0)
    inner_gate = jnp.zeros((ROWS, FSLICE), F32)
    inner_up = jnp.zeros((ROWS, FSLICE), F32)
    even_st = jnp.zeros((ROWS, 128), F32)
    odd_st = jnp.zeros((ROWS, 128), F32)
    low_half = iota((ROWS, 128), 1) < 64
    for dx in ARRIVAL:
        wait_for(recv_sem.at[5, dx], xall.at[rc], NY - 1 if dx == 0 else NY)
        part = xall.at[rc, chips_of(dx)]
        to_partner(8, part, part, dx)
    for dx in ARRIVAL:
        wait_for(recv_sem.at[8, dx], xall.at[rc], NY)
        base = first_of(dx)
        pieces = []
        for j in range(NY):
            even, odd_x = xall[0, base // 2 + j], xall[1, base // 2 + j]
            pieces += [even[:, 0:128], jnp.where(low_half, even[:, 128:256], odd_x[:, 0:128]), odd_x[:, 128:256]]
            even_st = even_st + even[:, 128:256].astype(F32)
            odd_st = odd_st + odd_x[:, 0:128].astype(F32)
        xs = jnp.concatenate(pieces, axis=1)
        rows = pl.ds(pl.multiple_of(base * WIDTH, PER_X * WIDTH), PER_X * WIDTH)
        inner_gate = inner_gate + dot(xs, wg[rows, :])
        inner_up = inner_up + dot(xs, wu[rows, :])
    st = pltpu.roll(even_st, 64, 1) + odd_st
    st = st + pltpu.roll(st, 112, 1) + pltpu.roll(st, 96, 1)
    lane128 = iota((ROWS, 128), 1)
    squares = jnp.sum(jnp.where(lane128 == 8, st, 0.0), axis=1, keepdims=True)
    inverse = lax.rsqrt(squares / D + EPS)
    pair = nt_dot(mine.astype(BF16), hot128[...].astype(BF16))
    logits = st * inverse
    own_logit = jnp.sum(jnp.where(lane128 == c, logits, 0.0), axis=1, keepdims=True)
    other = jnp.sum(jnp.where((pair > 0.0) & (lane128 != c), logits, 0.0), axis=1, keepdims=True)
    share = 1.0 / (1.0 + jnp.exp(other - own_logit))
    inner_gate = inner_gate * inverse
    inner_up = inner_up * inverse
    act = (inner_gate / (1.0 + jnp.exp(-inner_gate)) * inner_up * share).astype(BF16)
    asend2[...] = act
    to_partner(9, asend2, arecv2, 0)
    half = wd.at[:, pl.ds(0, FSLICE)]
    pltpu.make_async_copy(half, half, down_sem.at[0]).wait()
    pltpu.make_async_copy(half, half, down_sem.at[2]).wait()
    pltpu.make_async_copy(arecv2, arecv2, recv_sem.at[9, 0]).wait()
    other = arecv2[...]
    act = jnp.concatenate([jnp.where(rc == 0, act, other), jnp.where(rc == 0, other, act)], axis=1)
    for dx in FAR_FIRST:
        base = ((rx + dx) % NX) * NY
        for j in range(NY):
            ypair[base + j] = dot(act, wd[base + j]).astype(BF16)
        if dx == 0:
            yrec[chip] = ypair[chip]
        to_chips(6, lambda peer: ypair.at[peer], yrec.at[chip], dx)

    ysum = jnp.zeros((ROWS, WPAD), F32)
    for dx in NEAR_FIRST:
        wait_for(recv_sem.at[6, dx], yrec, NY - 1 if dx == 0 else NY)
        ysum = ysum + jnp.sum(yrec[chips_of(dx)].astype(F32), axis=0)
    ysum = jnp.where(rc == 0, ysum, pltpu.roll(ysum, WPAD - 64, 1))
    back = lax.dot_general(
        mine.astype(BF16), ysum.astype(BF16), (((0,), (0,)), ((), ())), preferred_element_type=F32
    )
    for i in range(NC):
        both = jnp.concatenate(
            [back[i * BLOCK : (i + 1) * BLOCK, 0:128], back[i * BLOCK : (i + 1) * BLOCK, 128:256]], axis=0
        )
        zsend[i] = both.astype(BF16)
    zrec[c] = zsend[c]
    to_col(7, lambda peer: zsend.at[peer], zrec)
    wait_for(recv_sem.at[7, 0], zrec, NC - 1)
    z = jnp.sum(zrec[...].astype(F32), axis=0)
    final = hres[...]
    out[:, 0:128] = (final[:, 0:128] + z[0:BLOCK]).astype(out.dtype)
    out[:, 128:WIDTH] = (final[:, 128:WIDTH] + z[BLOCK:, 0 : WIDTH - 128]).astype(out.dtype)

    wait_for(send_sem.at[0], qall, NR - 1)
    wait_for(send_sem.at[1], hrec, NC - 1)
    wait_for(send_sem.at[2], prec, NR - 1)
    wait_for(send_sem.at[3], aall, NR - 1)
    wait_for(send_sem.at[4], trec, NC - 1)
    wait_for(send_sem.at[5], yrec, CHIPS - 1)
    wait_for(send_sem.at[6], yrec, CHIPS - 1)
    wait_for(send_sem.at[8], yrec, CHIPS)
    pltpu.make_async_copy(arecv2, arecv2, send_sem.at[9]).wait()
    pltpu.make_async_copy(half, half, down_sem.at[1]).wait()
    wait_for(send_sem.at[7], zrec, NC - 1)


def body(
    hidden,
    queries,
    new_keys,
    new_values,
    cache_keys,
    cache_values,
    lengths,
    page_table,
    resident,
    prefix_keys,
    prefix_values,
    out_weight,
    norm_gain,
    router_weight,
    experts,
    gate_weight,
    up_weight,
    down_projection_weight,
):
    hbm = pl.BlockSpec(memory_space=pltpu.HBM)
    vmem = pl.BlockSpec(memory_space=pltpu.VMEM)
    return pl.pallas_call(
        kernel,
        out_shape=jax.ShapeDtypeStruct((BLOCK, WIDTH), BF16),
        in_specs=[hbm] * 18,
        out_specs=vmem,
        scratch_shapes=[
            pltpu.SMEM((2,), jnp.int32),
            pltpu.SMEM((SLOTS, NR), jnp.int32),
            pltpu.SMEM((2, BLOCK), jnp.int32),
            pltpu.VMEM((BLOCK, WIDTH), BF16),
            pltpu.VMEM((2, GROUP * HD), BF16),
            pltpu.VMEM((2, HD), BF16),
            pltpu.VMEM((2, HD), BF16),
            pltpu.VMEM((8, SEQS), jnp.int32),
            pltpu.VMEM((SLOTS, NR), jnp.int32),
            pltpu.VMEM((1, WIDTH), F32),
            pltpu.VMEM((EXPERTS, WIDTH), BF16),
            pltpu.VMEM((2, CTX, HD), BF16),
            pltpu.VMEM((2, CTX, HD), BF16),
            pltpu.VMEM((SLOTS, PAGE, HD), BF16),
            pltpu.VMEM((SLOTS, PAGE, HD), BF16),
            pltpu.VMEM((WIDTH, GROUP * HD), BF16),
            pltpu.VMEM((D, FSLICE), BF16),
            pltpu.VMEM((D, FSLICE), BF16),
            pltpu.VMEM((CHIPS, NCORE * FSLICE, WPAD), BF16),
            pltpu.VMEM((HROWS, HD), BF16),
            pltpu.VMEM((NR, HROWS, HD), BF16),
            pltpu.VMEM((NR, HROWS, HD), BF16),
            pltpu.VMEM((NR, HROWS, HD), BF16),
            pltpu.VMEM((HROWS, HD), BF16),
            pltpu.VMEM((NR, HROWS, HD), BF16),
            pltpu.VMEM((NC, ROWS, WPAD), BF16),
            pltpu.VMEM((NC, ROWS, WPAD), BF16),
            pltpu.VMEM((ROWS, WPAD), BF16),
            pltpu.VMEM((NCORE, CHIPS, ROWS, WPAD), BF16),
            pltpu.VMEM((ROWS, FSLICE), BF16),
            pltpu.VMEM((ROWS, FSLICE), BF16),
            pltpu.VMEM((CHIPS, ROWS, WPAD), BF16),
            pltpu.VMEM((CHIPS, ROWS, WPAD), BF16),
            pltpu.VMEM((NC, 2 * BLOCK, 128), BF16),
            pltpu.VMEM((NC, 2 * BLOCK, 128), BF16),
            pltpu.VMEM((EXPERTS, 128), F32),
            pltpu.VMEM((NC, EXPERTS, 128), F32),
            pltpu.VMEM((GROUP * 2 * PER_X, PER_X * HROWS), BF16),
            pltpu.VMEM((KEYS, SEQS), BF16),
            pltpu.VMEM((NC * ROWS, WPAD), BF16),
            pltpu.VMEM((128, 128), F32),
            pltpu.VMEM((WIDTH, WPAD), BF16),
            pltpu.VMEM((8, WPAD), F32),
            pltpu.VMEM((BLOCK, WPAD), F32),
            pltpu.VMEM((SEQS, WPAD), F32),
            pltpu.VMEM((SEQS, WPAD), F32),
            pltpu.VMEM((SEQS, GROUP * HD), BF16),
            pltpu.VMEM((BLOCK, WPAD), F32),
            pltpu.SemaphoreType.DMA((18,)),
            pltpu.SemaphoreType.DMA((3,)),
            pltpu.SemaphoreType.DMA((10,)),
            pltpu.SemaphoreType.DMA((10, NX)),
        ],
        compiler_params=pltpu.CompilerParams(
            collective_id=0, has_side_effects=True, vmem_limit_bytes=67043328
        ),
        name="layer",
    )(
        lengths,
        resident.T,
        experts.T,
        hidden,
        queries,
        new_keys,
        new_values,
        page_table.T,
        norm_gain.reshape(1, WIDTH),
        router_weight.T,
        cache_keys,
        cache_values,
        prefix_keys,
        prefix_values,
        out_weight.T,
        gate_weight,
        up_weight,
        down_projection_weight,
    )


def solution(mesh):
    in_specs = (
        P("col", "row"),
        P("row", "col"),
        P("row", "col"),
        P("row", "col"),
        P("row", None, "col"),
        P("row", None, "col"),
        P("row"),
        P(),
        P(),
        P("row", None, None, "col"),
        P("row", None, None, "col"),
        P("col", "row"),
        P("row"),
        P("row", None),
        P("col", None),
        P("col", None, "row"),
        P("col", None, "row"),
        P("col", "row", None),
    )
    return jax.shard_map(body, mesh=mesh, in_specs=in_specs, out_specs=P("col", "row"), check_vma=False)
```

```python
import functools
import math

import jax
import jax.numpy as jnp
from jax import lax
from jax.experimental import pallas as pl
from jax.experimental.pallas import tpu as pltpu
from jax.sharding import PartitionSpec as P

D = 6144
HQ = 48
KVH = 8
HD = 128
GROUP = HQ // KVH
EXPERTS = 8
CAP = 4
NEG = -1e30
EPS = 1e-05
NX, NY, NCORE = 4, 4, 2
NR = NX * NY * NCORE
NC = 8
SEQS = 64
BLOCK = SEQS // NC
SLOTS = 4
PAGE = 128
KEYS = SLOTS * PAGE
CTX = 2048
WIDTH = D // NR
WPAD = 256
FSLICE = 256
ROWS = NC * CAP
HROWS = 16
SCALE = 1.0 / math.sqrt(HD)
F32 = jnp.float32
BF16 = jnp.bfloat16

ROW_PEERS = [
    (dx, dy, dc)
    for dx in range(NX)
    for dy in range(NY)
    for dc in range(NCORE)
    if (dx, dy, dc) != (0, 0, 0)
]
ROW_PEERS.sort(key=lambda t: -(min(t[0], NX - t[0]) + min(t[1], NY - t[1]) + 0.5 * t[2]))
PER_X = NY * NCORE
RECV = (0, 20, 4, 21, 22, 8, 16, 23, 12, 24)
LOCAL = (0, 1, 2, 2, 3, 3, 4, 5, 5, 6, 7, 8, 9, 10, 11, 12, 13, 13)
NEAR_FIRST = (0, 1, 3, 2)
ARRIVAL = (2, 1, 3, 0)
ORDER1 = (0, 1, 3, 2)
ORDER2 = (0, 1, 3, 2)
ORDER3 = (2, 1, 3, 0)
FAR_FIRST = (2, 1, 3, 0)
CHIP_PEERS = [t for t in ROW_PEERS if t[2] == 0]
CHIPS = NX * NY
COL_PEERS = sorted(range(1, NC), key=lambda d: -min(d, NC - d))


def iota(shape, dim):
    return lax.broadcasted_iota(jnp.int32, shape, dim)


def nt_dot(a, b):
    return lax.dot_general(a, b, (((1,), (1,)), ((), ())), preferred_element_type=F32)


def dot(a, b):
    return jnp.dot(a, b, preferred_element_type=F32)


def kernel(
    lengths_h,
    resident_h,
    experts_h,
    hidden_h,
    queries_h,
    new_keys_h,
    new_values_h,
    page_table_h,
    gain_h,
    router_h,
    cache_keys,
    cache_values,
    prefix_keys,
    prefix_values,
    out_weight,
    gate_weight,
    up_weight,
    down_weight,
    out,
    lengths,
    resident_s,
    experts_s,
    hidden,
    queries,
    fresh_kv,
    page_table,
    resident,
    gain,
    router,
    kv,
    pkv,
    wo,
    wgu,
    wd,
    qsend,
    qall,
    psend,
    prec,
    asend,
    aall,
    tsend,
    trec,
    xsend,
    xall,
    asend2,
    arecv2,
    ypair,
    yrec,
    zsend,
    zrec,
    hsend,
    hrec,
    sel,
    cntk,
    disp,
    hot128,
    raug,
    gpad,
    hpad,
    hplaced,
    pbs,
    attended,
    hres,
    local_sem,
    down_sem,
    send_sem,
    recv_sem,
):
    r = lax.axis_index("row")
    c = lax.axis_index("col")
    rx, ry, rc = r // (NY * NCORE), (r // NCORE) % NY, r % NCORE

    def row_peer(t):
        dx, dy, dc = t
        return ((rx + dx) % NX) * (NY * NCORE) + ((ry + dy) % NY) * NCORE + (rc + dc) % NCORE

    def col_peer(d):
        return (c + d) % NC

    barrier = pltpu.get_barrier_semaphore()
    for t in ROW_PEERS:
        pl.semaphore_signal(barrier, inc=1, device_id={"row": row_peer(t), "col": c}, device_id_type=pl.DeviceIdType.MESH)
    for d in COL_PEERS:
        pl.semaphore_signal(barrier, inc=1, device_id={"row": r, "col": col_peer(d)}, device_id_type=pl.DeviceIdType.MESH)

    loads = [
        pltpu.make_async_copy(s, t, local_sem.at[LOCAL[i]])
        for i, (s, t) in enumerate(
            (
                (queries_h, queries),
                (experts_h, experts_s),
                (cache_keys, kv.at[0]),
                (cache_values, kv.at[1]),
                (prefix_keys.at[0], pkv.at[0]),
                (prefix_values.at[0], pkv.at[1]),
                (lengths_h, lengths),
                (new_keys_h, fresh_kv.at[0]),
                (new_values_h, fresh_kv.at[1]),
                (resident_h, resident_s),
                (resident_h, resident),
                (page_table_h, page_table),
                (router_h, router),
                (gain_h, gain),
                (hidden_h, hidden),
                (out_weight, wo),
                (gate_weight.at[0], wgu.at[0]),
                (up_weight.at[0], wgu.at[1]),
            )
        )
    ]
    loads += [
        pltpu.make_async_copy(
            down_weight.at[0, :, pl.ds(pl.multiple_of(2 * WIDTH * k + 128 * rc, 128), WPAD)],
            wd.at[k, pl.ds(pl.multiple_of(rc * FSLICE, FSLICE), FSLICE)],
            down_sem.at[0],
        )
        for k in range(CHIPS)
    ]
    for load in loads:
        load.start()

    def to_row(phase, src_of, dst, only=None):
        for t in ROW_PEERS:
            if only is not None and t[0] != only:
                continue
            peer = row_peer(t)
            pltpu.make_async_remote_copy(
                src_ref=src_of(peer),
                dst_ref=dst.at[r],
                send_sem=send_sem.at[phase],
                recv_sem=recv_sem.at[RECV[phase] + (0 if phase == 3 else (NX - t[0]) % NX)],
                device_id={"row": peer, "col": c},
                device_id_type=pl.DeviceIdType.MESH,
            ).start()

    def to_chips(phase, src_of, dst, only=None):
        for t in CHIP_PEERS:
            if only is not None and t[0] != only:
                continue
            peer = row_peer(t)
            pltpu.make_async_remote_copy(
                src_ref=src_of(peer // NCORE),
                dst_ref=dst,
                send_sem=send_sem.at[phase],
                recv_sem=recv_sem.at[RECV[phase] + (0 if phase == 3 else (NX - t[0]) % NX)],
                device_id={"row": peer, "col": c},
                device_id_type=pl.DeviceIdType.MESH,
            ).start()

    def to_partner(phase, src, dst, dx):
        pltpu.make_async_remote_copy(
            src_ref=src,
            dst_ref=dst,
            send_sem=send_sem.at[phase],
            recv_sem=recv_sem.at[RECV[phase] + dx],
            device_id={"row": row_peer((0, 0, 1)), "col": c},
            device_id_type=pl.DeviceIdType.MESH,
        ).start()

    def chips_of(dx):
        return pl.ds(((rx + dx) % NX) * NY, NY)

    def to_col(phase, src_of, dst):
        for d in COL_PEERS:
            peer = col_peer(d)
            pltpu.make_async_remote_copy(
                src_ref=src_of(peer),
                dst_ref=dst.at[c],
                send_sem=send_sem.at[phase],
                recv_sem=recv_sem.at[RECV[phase]],
                device_id={"row": r, "col": peer},
                device_id_type=pl.DeviceIdType.MESH,
            ).start()

    def wait_for(sem, buffer, count):
        part = buffer.at[pl.ds(0, count)]
        pltpu.make_async_copy(part, part, sem).wait()

    def both_here(i, buffer):
        pltpu.make_async_copy(buffer, buffer, local_sem.at[i]).wait()

    def first_of(dx):
        return ((rx + dx) % NX) * PER_X

    def group_here(phase, buffer, dx):
        wait_for(recv_sem.at[RECV[phase] + dx], buffer, PER_X - 1 if dx == 0 else PER_X)

    loads[0].wait()
    loads[1].wait()
    q = queries[...].astype(F32)
    qrows = jnp.concatenate(
        [q[:, g * HD : (g + 1) * HD] for g in range(GROUP)] + [jnp.zeros((HROWS - 2 * GROUP, HD), F32)], axis=0
    )
    q16 = qrows.astype(BF16)
    qsend[...] = q16
    qall[r] = q16
    e_i, b_i = iota((EXPERTS, 128), 0), iota((EXPERTS, 128), 1)
    hot = jnp.zeros((EXPERTS, 128), F32)
    for b in range(BLOCK):
        named = (e_i == experts_s[0, b]) | (e_i == experts_s[1, b])
        hot = jnp.where(named & (b_i == c * BLOCK + b), 1.0, hot)
    hsend[...] = hot
    hrec[c] = hot

    pl.semaphore_wait(barrier, len(ROW_PEERS) + len(COL_PEERS))
    to_row(0, lambda peer: qsend, qall)
    to_col(1, lambda peer: hsend, hrec)

    for k in range(CHIPS):
        pltpu.make_async_remote_copy(
            src_ref=down_weight.at[0, :, pl.ds(pl.multiple_of(2 * WIDTH * k + 128 * (1 - rc), 128), WPAD)],
            dst_ref=wd.at[k, pl.ds(pl.multiple_of(rc * FSLICE, FSLICE), FSLICE)],
            send_sem=down_sem.at[1],
            recv_sem=down_sem.at[2],
            device_id={"row": row_peer((0, 0, 1)), "col": c},
            device_id_type=pl.DeviceIdType.MESH,
        ).start()

    for i in range(9, 15):
        loads[i].wait()
    table = page_table[...]
    res = resident[...]
    flat = iota(res.shape, 1) * SLOTS + iota(res.shape, 0)
    for j in range(SLOTS):
        page = resident_s[j, r]
        earlier = jnp.sum(jnp.where((res == page) & (flat < r * SLOTS + j), 1.0, 0.0), keepdims=True)
        times = jnp.where((table == page) & (earlier == 0.0), 1.0, 0.0)
        cntk[j * PAGE : (j + 1) * PAGE, :] = jnp.broadcast_to(jnp.sum(times, axis=0, keepdims=True), (PAGE, SEQS)).astype(BF16)
    want, have = iota((GROUP * 2 * PER_X, PER_X * HROWS), 0), iota((GROUP * 2 * PER_X, PER_X * HROWS), 1)
    token = want % (2 * PER_X)
    there = (token // 2) * HROWS + 2 * (want // (2 * PER_X)) + token % 2
    sel[...] = jnp.where(have == there, 1.0, 0.0).astype(BF16)
    here = jnp.where(iota((SEQS, BLOCK), 0) == c * BLOCK + iota((SEQS, BLOCK), 1), 1.0, 0.0).astype(BF16)
    place = jnp.where(
        (iota((EXPERTS, WPAD), 1) >= WIDTH) & (iota((EXPERTS, WPAD), 1) < WIDTH + 48)
        & ((iota((EXPERTS, WPAD), 1) - WIDTH) % 16 == iota((EXPERTS, WPAD), 0)), 1.0, 0.0
    ).astype(BF16)
    raug[...] = lax.dot_general(router[...], place, (((0,), (0,)), ((), ())), preferred_element_type=F32).astype(BF16)
    gpad[...] = jnp.zeros_like(gpad)
    gpad[0:1, 0:WIDTH] = gain[...]
    hpad[...] = jnp.zeros_like(hpad)
    hpad[:, 0:WIDTH] = hidden[...].astype(F32)
    hplaced[...] = dot(here, hpad[...].astype(BF16))
    pbs[...] = jnp.zeros_like(pbs)
    hot128[...] = jnp.zeros_like(hot128)

    loads[6].wait()
    both_here(5, fresh_kv)
    both_here(2, kv)
    odd = iota((HROWS, 1), 0) % 2 == 1
    own = [nt_dot(q16, kv[0, s]) for s in range(2)]
    scores = jnp.where(odd, own[1], own[0]) * SCALE
    length = jnp.where(odd, lengths[1], lengths[0])
    scores = jnp.where(iota((HROWS, CTX), 1) < length, scores, NEG)
    fresh_k = jnp.where(odd, fresh_kv[0, 1:2, :].astype(F32), fresh_kv[0, 0:1, :].astype(F32))
    fresh_v = jnp.where(odd, fresh_kv[1, 1:2, :].astype(F32), fresh_kv[1, 0:1, :].astype(F32))
    fresh = jnp.sum(qrows * fresh_k, axis=1, keepdims=True) * SCALE
    peak = jnp.maximum(jnp.max(scores, axis=1, keepdims=True), fresh)
    expo = jnp.exp(scores - peak)
    fresh_e = jnp.exp(fresh - peak)
    own_total = jnp.sum(expo, axis=1, keepdims=True) + fresh_e
    mixed = (
        dot(jnp.where(odd, 0.0, expo).astype(BF16), kv[1, 0])
        + dot(jnp.where(odd, expo, 0.0).astype(BF16), kv[1, 1])
        + fresh_e.astype(BF16).astype(F32) * fresh_v
    )
    own_peak = peak

    both_here(3, pkv)
    n = PER_X * HROWS
    k_i = iota((n, HD), 0) % HROWS
    seq = (iota((n, SEQS), 0) // HROWS) * 2 + iota((n, SEQS), 0) % 2
    for dx in ORDER1:
        group_here(0, qall, dx)
        base = first_of(dx)
        qs = qall[pl.ds(base, PER_X)].reshape(n, HD)
        member = seq + 2 * base == iota((n, SEQS), 1)
        times = nt_dot(jnp.where(member, 1.0, 0.0).astype(BF16), cntk[...])
        sc = nt_dot(qs, pkv[0].reshape(KEYS, HD)) * SCALE
        sc = jnp.where(times > 0.0, sc, NEG)
        m = jnp.max(sc, axis=1, keepdims=True)
        e = jnp.exp(sc - m) * times
        l = jnp.sum(e, axis=1, keepdims=True)
        o = dot(e.astype(BF16), pkv[1].reshape(KEYS, HD))
        some = l > 0.0
        safe = jnp.where(some, l, 1.0)
        o = o / safe
        lse = jnp.where(some, m + jnp.log(safe), NEG)
        diag = jnp.where(k_i == iota((n, HD), 1), lse, 0.0)
        across = jnp.sum(diag.reshape(PER_X, HROWS, HD), axis=1, keepdims=True)
        across = jnp.broadcast_to(across, (PER_X, HROWS, HD)).reshape(n, HD)
        hi = across.astype(BF16).astype(F32)
        mid = (across - hi).astype(BF16).astype(F32)
        lo = across - hi - mid
        tail = jnp.where(k_i == 12, hi, jnp.where(k_i == 13, mid, jnp.where(k_i == 14, lo, 0.0)))
        psend[pl.ds(base, PER_X)] = jnp.where(k_i < 12, o, tail).astype(BF16).reshape(PER_X, HROWS, HD)
        if dx == 0:
            prec[r] = psend[r]
        to_row(2, lambda peer: psend.at[peer], prec, dx)

    wait_for(recv_sem.at[RECV[1]], hrec, NC - 1)
    hot = jnp.sum(hrec[...], axis=0)
    hot128[0:EXPERTS, :] = hot
    u0, u1 = iota((128, 128), 0), iota((128, 128), 1)
    before = jnp.where((u0 < u1) & (u0 // BLOCK == u1 // BLOCK), 1.0, 0.0).astype(BF16)
    rank = dot(hot.astype(BF16), before)
    d_r, d_l = iota((ROWS, 128), 0), iota((ROWS, 128), 1)
    for e in range(EXPERTS):
        hit = (
            (hot[e : e + 1, :] > 0.0)
            & (rank[e : e + 1, :] == (d_r % CAP).astype(F32))
            & (d_l // BLOCK == d_r // CAP)
        )
        home = d_l % SEQS == e * BLOCK + d_r % BLOCK
        low = jnp.where(hit & (d_l < SEQS), 1.0, 0.0) + jnp.where(
            home & (d_l >= SEQS) & (d_r // BLOCK == 0), 1.0, 0.0
        )
        high = jnp.where(home & (d_r // BLOCK == 1 + d_l // SEQS), 1.0, 0.0)
        disp[e * ROWS : (e + 1) * ROWS, 0:128] = low.astype(BF16)
        disp[e * ROWS : (e + 1) * ROWS, 128:256] = high.astype(BF16)

    on_diag = iota((PER_X, HROWS, HD), 1) == iota((PER_X, HROWS, HD), 2)
    real = iota((PER_X, HROWS, 1), 1) < 12
    merged = [(own_peak, own_total, mixed)]
    for dx in ORDER2:
        group_here(2, prec, dx)
        parts = prec[pl.ds(first_of(dx), PER_X)].astype(F32)
        lrow = parts[:, 12:13, :] + parts[:, 13:14, :] + parts[:, 14:15, :]
        lse = jnp.sum(jnp.where(on_diag, jnp.broadcast_to(lrow, parts.shape), 0.0), axis=2, keepdims=True)
        lse = jnp.where(real, lse, NEG)
        top = jnp.max(lse, axis=0)
        w = jnp.exp(lse - top[None])
        w = jnp.where(lse > 0.5 * NEG, w, 0.0)
        merged.append((top, jnp.sum(w, axis=0), jnp.sum(w * parts, axis=0)))
    top = functools.reduce(jnp.maximum, [m for m, _, _ in merged])
    ws = [jnp.exp(m - top) for m, _, _ in merged]
    total = sum(w * l for w, (_, l, _) in zip(ws, merged))
    mixed = sum(w * o for w, (_, _, o) in zip(ws, merged))
    att = jnp.where(iota((HROWS, HD), 0) < 12, mixed / total, 0.0).astype(BF16)
    asend[...] = att
    aall[r] = att
    to_row(3, lambda peer: asend, aall)

    loads[15].wait()
    wait_for(recv_sem.at[RECV[3]], aall, NR - 1)
    for dx in range(NX):
        base = dx * PER_X
        picked = dot(sel[...], aall[pl.ds(base, PER_X)].reshape(PER_X * HROWS, HD)).astype(BF16)
        tokens = 2 * PER_X
        heads = jnp.concatenate([picked[g * tokens : (g + 1) * tokens] for g in range(GROUP)], axis=1)
        attended[pl.ds(pl.multiple_of(2 * base, tokens), tokens), :] = heads
    pbs[:, 0:WIDTH] = nt_dot(attended[...], wo[...])
    plain = pbs[...]
    with_hidden = plain + hplaced[...]
    lane = iota((SEQS, WPAD), 1)
    moved = [jnp.where(lane >= WIDTH, pltpu.roll(plain, WIDTH - 64 * i, 1), 0.0) for i in range(3)]
    stacked = jnp.concatenate([with_hidden] + moved, axis=0).astype(BF16)
    tsend[...] = dot(disp[...], stacked).astype(BF16).reshape(NC, ROWS, WPAD)
    trec[c] = tsend[c]
    to_col(4, lambda peer: tsend.at[peer], trec)

    wait_for(recv_sem.at[RECV[4]], trec, NC - 1)
    resid = jnp.sum(trec[...].astype(F32), axis=0)
    lane8 = iota((BLOCK, WPAD), 1)
    home = hpad[...]
    for i in range(3):
        piece = pltpu.roll(resid[i * BLOCK : (i + 1) * BLOCK, :], (64 * i + 64) % WPAD, 1)
        home = home + jnp.where(lane8 // 64 == i, piece, 0.0)
    hres[...] = home
    lane32 = iota((ROWS, WPAD), 1)
    squares = jnp.sum(jnp.where(lane32 < WIDTH, resid * resid, 0.0), axis=1, keepdims=True)
    x = resid * gpad[0:1, :]
    stats = dot(x[:, 0:WIDTH].astype(BF16), raug[...])
    stats = stats + jnp.where((lane32 >= WIDTH) & ((lane32 - WIDTH) % 16 == 8), squares, 0.0)
    hi = stats.astype(BF16).astype(F32)
    mid = (stats - hi).astype(BF16).astype(F32)
    lo = stats - hi - mid
    x = jnp.where(lane32 < WIDTH, x, jnp.where(lane32 < WIDTH + 16, hi, jnp.where(lane32 < WIDTH + 32, mid, jnp.where(lane32 < WIDTH + 48, lo, 0.0))))
    x = jnp.where(rc == 0, x, pltpu.roll(x, 64, 1)).astype(BF16)
    xsend[...] = x
    chip = r // NCORE
    xall[rc, chip] = x
    to_chips(5, lambda peer: xsend, xall.at[rc, chip])

    both_here(13, wgu)
    mine = disp[pl.ds(pl.multiple_of(c * ROWS, ROWS), ROWS), 0:128]
    mine = jnp.where(iota((ROWS, 128), 1) < SEQS, mine.astype(F32), 0.0)
    inner_gate = jnp.zeros((ROWS, FSLICE), F32)
    inner_up = jnp.zeros((ROWS, FSLICE), F32)
    even_st = jnp.zeros((ROWS, 128), F32)
    odd_st = jnp.zeros((ROWS, 128), F32)
    low_half = iota((ROWS, 128), 1) < 64
    for dx in ARRIVAL:
        wait_for(recv_sem.at[RECV[5] + dx], xall.at[rc], NY - 1 if dx == 0 else NY)
        part = xall.at[rc, chips_of(dx)]
        to_partner(8, part, part, dx)
    for dx in ARRIVAL:
        wait_for(recv_sem.at[RECV[8] + dx], xall.at[rc], NY)
        base = first_of(dx)
        pieces = []
        for j in range(NY):
            even, odd_x = xall[0, base // 2 + j], xall[1, base // 2 + j]
            pieces += [even[:, 0:128], jnp.where(low_half, even[:, 128:256], odd_x[:, 0:128]), odd_x[:, 128:256]]
            even_st = even_st + even[:, 128:256].astype(F32)
            odd_st = odd_st + odd_x[:, 0:128].astype(F32)
        xs = jnp.concatenate(pieces, axis=1)
        rows = pl.ds(pl.multiple_of(base * WIDTH, PER_X * WIDTH), PER_X * WIDTH)
        inner_gate = inner_gate + dot(xs, wgu[0, rows, :])
        inner_up = inner_up + dot(xs, wgu[1, rows, :])
    st = pltpu.roll(even_st, 64, 1) + odd_st
    st = st + pltpu.roll(st, 112, 1) + pltpu.roll(st, 96, 1)
    lane128 = iota((ROWS, 128), 1)
    squares = jnp.sum(jnp.where(lane128 == 8, st, 0.0), axis=1, keepdims=True)
    inverse = lax.rsqrt(squares / D + EPS)
    pair = nt_dot(mine.astype(BF16), hot128[...].astype(BF16))
    logits = st * inverse
    own_logit = jnp.sum(jnp.where(lane128 == c, logits, 0.0), axis=1, keepdims=True)
    other = jnp.sum(jnp.where((pair > 0.0) & (lane128 != c), logits, 0.0), axis=1, keepdims=True)
    share = 1.0 / (1.0 + jnp.exp(other - own_logit))
    inner_gate = inner_gate * inverse
    inner_up = inner_up * inverse
    act = (inner_gate / (1.0 + jnp.exp(-inner_gate)) * inner_up * share).astype(BF16)
    asend2[...] = act
    to_partner(9, asend2, arecv2, 0)
    half = wd.at[:, pl.ds(0, FSLICE)]
    pltpu.make_async_copy(half, half, down_sem.at[0]).wait()
    pltpu.make_async_copy(half, half, down_sem.at[2]).wait()
    pltpu.make_async_copy(arecv2, arecv2, recv_sem.at[RECV[9]]).wait()
    other = arecv2[...]
    act = jnp.concatenate([jnp.where(rc == 0, act, other), jnp.where(rc == 0, other, act)], axis=1)
    for dx in FAR_FIRST:
        base = ((rx + dx) % NX) * NY
        for j in range(NY):
            ypair[base + j] = dot(act, wd[base + j]).astype(BF16)
        if dx == 0:
            yrec[chip] = ypair[chip]
        to_chips(6, lambda peer: ypair.at[peer], yrec.at[chip], dx)

    ysum = jnp.zeros((ROWS, WPAD), F32)
    for dx in NEAR_FIRST:
        wait_for(recv_sem.at[RECV[6] + dx], yrec, NY - 1 if dx == 0 else NY)
        ysum = ysum + jnp.sum(yrec[chips_of(dx)].astype(F32), axis=0)
    ysum = jnp.where(rc == 0, ysum, pltpu.roll(ysum, WPAD - 64, 1))
    back = lax.dot_general(
        mine.astype(BF16), ysum.astype(BF16), (((0,), (0,)), ((), ())), preferred_element_type=F32
    )
    for i in range(NC):
        both = jnp.concatenate(
            [back[i * BLOCK : (i + 1) * BLOCK, 0:128], back[i * BLOCK : (i + 1) * BLOCK, 128:256]], axis=0
        )
        zsend[i] = both.astype(BF16)
    zrec[c] = zsend[c]
    to_col(7, lambda peer: zsend.at[peer], zrec)
    wait_for(recv_sem.at[RECV[7]], zrec, NC - 1)
    z = jnp.sum(zrec[...].astype(F32), axis=0)
    final = hres[...]
    out[:, 0:128] = (final[:, 0:128] + z[0:BLOCK]).astype(out.dtype)
    out[:, 128:WIDTH] = (final[:, 128:WIDTH] + z[BLOCK:, 0 : WIDTH - 128]).astype(out.dtype)

    wait_for(send_sem.at[0], qall, NR - 1)
    wait_for(send_sem.at[1], hrec, NC - 1)
    wait_for(send_sem.at[2], prec, NR - 1)
    wait_for(send_sem.at[3], aall, NR - 1)
    wait_for(send_sem.at[4], trec, NC - 1)
    wait_for(send_sem.at[5], yrec, CHIPS - 1)
    wait_for(send_sem.at[6], yrec, CHIPS - 1)
    wait_for(send_sem.at[8], yrec, CHIPS)
    pltpu.make_async_copy(arecv2, arecv2, send_sem.at[9]).wait()
    pltpu.make_async_copy(half, half, down_sem.at[1]).wait()
    wait_for(send_sem.at[7], zrec, NC - 1)


def body(
    hidden,
    queries,
    new_keys,
    new_values,
    cache_keys,
    cache_values,
    lengths,
    page_table,
    resident,
    prefix_keys,
    prefix_values,
    out_weight,
    norm_gain,
    router_weight,
    experts,
    gate_weight,
    up_weight,
    down_projection_weight,
):
    hbm = pl.BlockSpec(memory_space=pltpu.HBM)
    vmem = pl.BlockSpec(memory_space=pltpu.VMEM)
    operands = (
        lengths,
        resident.T,
        experts.T,
        hidden,
        queries,
        new_keys,
        new_values,
        page_table.T,
        norm_gain.reshape(1, WIDTH),
        router_weight.T,
        cache_keys,
        cache_values,
        prefix_keys,
        prefix_values,
        out_weight.T,
        gate_weight,
        up_weight,
        down_projection_weight,
    )
    return pl.pallas_call(
        kernel,
        out_shape=jax.ShapeDtypeStruct((BLOCK, WIDTH), BF16),
        in_specs=[hbm] * 18,
        out_specs=vmem,
        scratch_shapes=[
            pltpu.SMEM((2,), jnp.int32),
            pltpu.SMEM((SLOTS, NR), jnp.int32),
            pltpu.SMEM((2, BLOCK), jnp.int32),
            pltpu.VMEM((BLOCK, WIDTH), BF16),
            pltpu.VMEM((2, GROUP * HD), BF16),
            pltpu.VMEM((2, 2, HD), BF16),
            pltpu.VMEM((8, SEQS), jnp.int32),
            pltpu.VMEM((SLOTS, NR), jnp.int32),
            pltpu.VMEM((1, WIDTH), F32),
            pltpu.VMEM((EXPERTS, WIDTH), BF16),
            pltpu.VMEM((2, 2, CTX, HD), BF16),
            pltpu.VMEM((2, SLOTS, PAGE, HD), BF16),
            pltpu.VMEM((WIDTH, GROUP * HD), BF16),
            pltpu.VMEM((2, D, FSLICE), BF16),
            pltpu.VMEM((CHIPS, NCORE * FSLICE, WPAD), BF16),
            pltpu.VMEM((HROWS, HD), BF16),
            pltpu.VMEM((NR, HROWS, HD), BF16),
            pltpu.VMEM((NR, HROWS, HD), BF16),
            pltpu.VMEM((NR, HROWS, HD), BF16),
            pltpu.VMEM((HROWS, HD), BF16),
            pltpu.VMEM((NR, HROWS, HD), BF16),
            pltpu.VMEM((NC, ROWS, WPAD), BF16),
            pltpu.VMEM((NC, ROWS, WPAD), BF16),
            pltpu.VMEM((ROWS, WPAD), BF16),
            pltpu.VMEM((NCORE, CHIPS, ROWS, WPAD), BF16),
            pltpu.VMEM((ROWS, FSLICE), BF16),
            pltpu.VMEM((ROWS, FSLICE), BF16),
            pltpu.VMEM((CHIPS, ROWS, WPAD), BF16),
            pltpu.VMEM((CHIPS, ROWS, WPAD), BF16),
            pltpu.VMEM((NC, 2 * BLOCK, 128), BF16),
            pltpu.VMEM((NC, 2 * BLOCK, 128), BF16),
            pltpu.VMEM((EXPERTS, 128), F32),
            pltpu.VMEM((NC, EXPERTS, 128), F32),
            pltpu.VMEM((GROUP * 2 * PER_X, PER_X * HROWS), BF16),
            pltpu.VMEM((KEYS, SEQS), BF16),
            pltpu.VMEM((NC * ROWS, WPAD), BF16),
            pltpu.VMEM((128, 128), F32),
            pltpu.VMEM((WIDTH, WPAD), BF16),
            pltpu.VMEM((8, WPAD), F32),
            pltpu.VMEM((BLOCK, WPAD), F32),
            pltpu.VMEM((SEQS, WPAD), F32),
            pltpu.VMEM((SEQS, WPAD), F32),
            pltpu.VMEM((SEQS, GROUP * HD), BF16),
            pltpu.VMEM((BLOCK, WPAD), F32),
            pltpu.SemaphoreType.DMA((14,)),
            pltpu.SemaphoreType.DMA((3,)),
            pltpu.SemaphoreType.DMA((10,)),
            pltpu.SemaphoreType.DMA((25,)),
        ],
        compiler_params=pltpu.CompilerParams(
            collective_id=0, has_side_effects=True, vmem_limit_bytes=40 * 1024 * 1024
        ),
        name="layer",
    )(*[pltpu.with_memory_space_constraint(a, pltpu.HBM) for a in operands])


def solution(mesh):
    in_specs = (
        P("col", "row"),
        P("row", "col"),
        P("row", "col"),
        P("row", "col"),
        P("row", None, "col"),
        P("row", None, "col"),
        P("row"),
        P(),
        P(),
        P("row", None, None, "col"),
        P("row", None, None, "col"),
        P("col", "row"),
        P("row"),
        P("row", None),
        P("col", None),
        P("col", None, "row"),
        P("col", None, "row"),
        P("col", "row", None),
    )
    return jax.shard_map(body, mesh=mesh, in_specs=in_specs, out_specs=P("col", "row"), check_vma=False)
```

```python
import functools
import math

import jax
import jax.numpy as jnp
from jax import lax
from jax.experimental import pallas as pl
from jax.experimental.pallas import tpu as pltpu
from jax.sharding import PartitionSpec as P

D = 6144
HQ = 48
KVH = 8
HD = 128
GROUP = HQ // KVH
EXPERTS = 8
CAP = 4
NEG = -1e30
EPS = 1e-05
NX, NY, NCORE = 4, 4, 2
NR = NX * NY * NCORE
NC = 8
SEQS = 64
BLOCK = SEQS // NC
SLOTS = 4
PAGE = 128
KEYS = SLOTS * PAGE
CTX = 2048
WIDTH = D // NR
WPAD = 256
FSLICE = 256
ROWS = NC * CAP
HROWS = 16
SCALE = 1.0 / math.sqrt(HD)
F32 = jnp.float32
BF16 = jnp.bfloat16

ROW_PEERS = [
    (dx, dy, dc)
    for dx in range(NX)
    for dy in range(NY)
    for dc in range(NCORE)
    if (dx, dy, dc) != (0, 0, 0)
]
ROW_PEERS.sort(key=lambda t: -(min(t[0], NX - t[0]) + min(t[1], NY - t[1]) + 0.5 * t[2]))
PER_X = NY * NCORE
RECV = (0, 20, 4, 21, 22, 8, 16, 23, 12, 24)
LOCAL = (0, 1, 2, 2, 3, 3, 4, 5, 5, 6, 7, 8, 9, 10, 11, 12)
NEAR_FIRST = (0, 1, 3, 2)
ARRIVAL = (2, 1, 3, 0)
ORDER1 = (0, 1, 3, 2)
ORDER2 = (0, 1, 3, 2)
ORDER3 = (2, 1, 3, 0)
FAR_FIRST = (2, 1, 3, 0)
CHIP_PEERS = [t for t in ROW_PEERS if t[2] == 0]
CHIPS = NX * NY
COL_PEERS = sorted(range(1, NC), key=lambda d: -min(d, NC - d))


def iota(shape, dim):
    return lax.broadcasted_iota(jnp.int32, shape, dim)


def nt_dot(a, b):
    return lax.dot_general(a, b, (((1,), (1,)), ((), ())), preferred_element_type=F32)


def dot(a, b):
    return jnp.dot(a, b, preferred_element_type=F32)


def kernel(
    lengths_h,
    resident_h,
    experts_h,
    hidden_h,
    queries_h,
    new_keys_h,
    new_values_h,
    page_table_h,
    gain_h,
    router_h,
    cache_keys,
    cache_values,
    prefix_keys,
    prefix_values,
    out_weight,
    gate_weight,
    up_weight,
    down_weight,
    out,
    lengths,
    resident_s,
    experts_s,
    hidden,
    queries,
    fresh_kv,
    page_table,
    resident,
    gain,
    router,
    kv,
    pkv,
    wo,
    wx,
    wd,
    qsend,
    qall,
    psend,
    prec,
    asend,
    aall,
    tsend,
    trec,
    xsend,
    xall,
    insend,
    inrecv,
    stsend,
    strecv,
    ypair,
    yrec,
    zsend,
    zrec,
    hsend,
    hrec,
    sel,
    cntk,
    disp,
    hot128,
    raug,
    gpad,
    hpad,
    hplaced,
    pbs,
    attended,
    hres,
    local_sem,
    down_sem,
    send_sem,
    recv_sem,
):
    r = lax.axis_index("row")
    c = lax.axis_index("col")
    rx, ry, rc = r // (NY * NCORE), (r // NCORE) % NY, r % NCORE

    def row_peer(t):
        dx, dy, dc = t
        return ((rx + dx) % NX) * (NY * NCORE) + ((ry + dy) % NY) * NCORE + (rc + dc) % NCORE

    def col_peer(d):
        return (c + d) % NC

    barrier = pltpu.get_barrier_semaphore()
    for t in ROW_PEERS:
        pl.semaphore_signal(barrier, inc=1, device_id={"row": row_peer(t), "col": c}, device_id_type=pl.DeviceIdType.MESH)
    for d in COL_PEERS:
        pl.semaphore_signal(barrier, inc=1, device_id={"row": r, "col": col_peer(d)}, device_id_type=pl.DeviceIdType.MESH)

    loads = [
        pltpu.make_async_copy(s, t, local_sem.at[LOCAL[i]])
        for i, (s, t) in enumerate(
            (
                (queries_h, queries),
                (experts_h, experts_s),
                (cache_keys, kv.at[0]),
                (cache_values, kv.at[1]),
                (prefix_keys.at[0], pkv.at[0]),
                (prefix_values.at[0], pkv.at[1]),
                (lengths_h, lengths),
                (new_keys_h, fresh_kv.at[0]),
                (new_values_h, fresh_kv.at[1]),
                (resident_h, resident_s),
                (resident_h, resident),
                (page_table_h, page_table),
                (router_h, router),
                (gain_h, gain),
                (hidden_h, hidden),
                (out_weight, wo),
            )
        )
    ]
    loads += [
        pltpu.make_async_copy(
            down_weight.at[0, :, pl.ds(pl.multiple_of(2 * WIDTH * k + 128 * rc, 128), WPAD)],
            wd.at[pl.ds(0, FSLICE), pl.ds(k * WPAD, WPAD)],
            down_sem.at[0],
        )
        for k in range(CHIPS)
    ]
    loads += [
        pltpu.make_async_copy(
            w.at[0, pl.ds(pl.multiple_of(2 * WIDTH * k + WIDTH * rc, 64), WIDTH), :],
            wx.at[pl.ds(k * WIDTH, WIDTH), pl.ds(2 * i * FSLICE, FSLICE)],
            down_sem.at[3],
        )
        for k in range(CHIPS)
        for i, w in enumerate((gate_weight, up_weight))
    ]
    loads[0].start()
    loads[1].start()

    def to_row(phase, src_of, dst, only=None):
        for t in ROW_PEERS:
            if only is not None and t[0] != only:
                continue
            peer = row_peer(t)
            pltpu.make_async_remote_copy(
                src_ref=src_of(peer),
                dst_ref=dst.at[r],
                send_sem=send_sem.at[phase],
                recv_sem=recv_sem.at[RECV[phase] + (0 if phase == 3 else (NX - t[0]) % NX)],
                device_id={"row": peer, "col": c},
                device_id_type=pl.DeviceIdType.MESH,
            ).start()

    def to_chips(phase, src_of, dst, only=None):
        for t in CHIP_PEERS:
            if only is not None and t[0] != only:
                continue
            peer = row_peer(t)
            pltpu.make_async_remote_copy(
                src_ref=src_of(peer // NCORE),
                dst_ref=dst,
                send_sem=send_sem.at[phase],
                recv_sem=recv_sem.at[RECV[phase] + (0 if phase == 3 else (NX - t[0]) % NX)],
                device_id={"row": peer, "col": c},
                device_id_type=pl.DeviceIdType.MESH,
            ).start()

    def to_partner(phase, src, dst, dx):
        pltpu.make_async_remote_copy(
            src_ref=src,
            dst_ref=dst,
            send_sem=send_sem.at[phase],
            recv_sem=recv_sem.at[RECV[phase] + dx],
            device_id={"row": row_peer((0, 0, 1)), "col": c},
            device_id_type=pl.DeviceIdType.MESH,
        ).start()

    def chips_of(dx):
        return pl.ds(((rx + dx) % NX) * NY, NY)

    def to_col(phase, src_of, dst):
        for d in COL_PEERS:
            peer = col_peer(d)
            pltpu.make_async_remote_copy(
                src_ref=src_of(peer),
                dst_ref=dst.at[c],
                send_sem=send_sem.at[phase],
                recv_sem=recv_sem.at[RECV[phase]],
                device_id={"row": r, "col": peer},
                device_id_type=pl.DeviceIdType.MESH,
            ).start()

    def wait_for(sem, buffer, count):
        part = buffer.at[pl.ds(0, count)]
        pltpu.make_async_copy(part, part, sem).wait()

    def both_here(i, buffer):
        pltpu.make_async_copy(buffer, buffer, local_sem.at[i]).wait()

    def first_of(dx):
        return ((rx + dx) % NX) * PER_X

    def group_here(phase, buffer, dx):
        wait_for(recv_sem.at[RECV[phase] + dx], buffer, PER_X - 1 if dx == 0 else PER_X)

    loads[0].wait()
    loads[1].wait()
    for load in loads[2:16]:
        load.start()
    q = queries[...].astype(F32)
    qrows = jnp.concatenate(
        [q[:, g * HD : (g + 1) * HD] for g in range(GROUP)] + [jnp.zeros((HROWS - 2 * GROUP, HD), F32)], axis=0
    )
    q16 = qrows.astype(BF16)
    qsend[...] = q16
    qall[r] = q16
    e_i, b_i = iota((EXPERTS, 128), 0), iota((EXPERTS, 128), 1)
    hot = jnp.zeros((EXPERTS, 128), F32)
    for b in range(BLOCK):
        named = (e_i == experts_s[0, b]) | (e_i == experts_s[1, b])
        hot = jnp.where(named & (b_i == c * BLOCK + b), 1.0, hot)
    hsend[...] = hot
    hrec[c] = hot

    pl.semaphore_wait(barrier, len(ROW_PEERS) + len(COL_PEERS))
    to_row(0, lambda peer: qsend, qall)
    to_col(1, lambda peer: hsend, hrec)

    for load in loads[16:]:
        load.start()
    for k in range(CHIPS):
        for i, w in enumerate((gate_weight, up_weight)):
            pltpu.make_async_remote_copy(
                src_ref=w.at[0, pl.ds(pl.multiple_of(2 * WIDTH * k + WIDTH * (1 - rc), 64), WIDTH), :],
                dst_ref=wx.at[pl.ds(k * WIDTH, WIDTH), pl.ds((2 * i + 1) * FSLICE, FSLICE)],
                send_sem=down_sem.at[4],
                recv_sem=down_sem.at[5],
                device_id={"row": row_peer((0, 0, 1)), "col": c},
                device_id_type=pl.DeviceIdType.MESH,
            ).start()
    for k in range(CHIPS):
        pltpu.make_async_remote_copy(
            src_ref=down_weight.at[0, :, pl.ds(pl.multiple_of(2 * WIDTH * k + 128 * (1 - rc), 128), WPAD)],
            dst_ref=wd.at[pl.ds(FSLICE, FSLICE), pl.ds(k * WPAD, WPAD)],
            send_sem=down_sem.at[1],
            recv_sem=down_sem.at[2],
            device_id={"row": row_peer((0, 0, 1)), "col": c},
            device_id_type=pl.DeviceIdType.MESH,
        ).start()

    for i in range(9, 15):
        loads[i].wait()
    table = page_table[...]
    res = resident[...]
    flat = iota(res.shape, 1) * SLOTS + iota(res.shape, 0)
    for j in range(SLOTS):
        page = resident_s[j, r]
        earlier = jnp.sum(jnp.where((res == page) & (flat < r * SLOTS + j), 1.0, 0.0), keepdims=True)
        times = jnp.where((table == page) & (earlier == 0.0), 1.0, 0.0)
        cntk[j * PAGE : (j + 1) * PAGE, :] = jnp.broadcast_to(jnp.sum(times, axis=0, keepdims=True), (PAGE, SEQS)).astype(BF16)
    want, have = iota((GROUP * 2 * PER_X, PER_X * HROWS), 0), iota((GROUP * 2 * PER_X, PER_X * HROWS), 1)
    token = want % (2 * PER_X)
    there = (token // 2) * HROWS + 2 * (want // (2 * PER_X)) + token % 2
    sel[...] = jnp.where(have == there, 1.0, 0.0).astype(BF16)
    here = jnp.where(iota((SEQS, BLOCK), 0) == c * BLOCK + iota((SEQS, BLOCK), 1), 1.0, 0.0).astype(BF16)
    place = jnp.where(
        (iota((EXPERTS, WPAD), 1) >= WIDTH) & (iota((EXPERTS, WPAD), 1) < WIDTH + 48)
        & ((iota((EXPERTS, WPAD), 1) - WIDTH) % 16 == iota((EXPERTS, WPAD), 0)), 1.0, 0.0
    ).astype(BF16)
    raug[...] = lax.dot_general(router[...], place, (((0,), (0,)), ((), ())), preferred_element_type=F32).astype(BF16)
    gpad[...] = jnp.zeros_like(gpad)
    gpad[0:1, 0:WIDTH] = gain[...]
    hpad[...] = jnp.zeros_like(hpad)
    hpad[:, 0:WIDTH] = hidden[...].astype(F32)
    hplaced[...] = dot(here, hpad[...].astype(BF16))
    pbs[...] = jnp.zeros_like(pbs)
    hot128[...] = jnp.zeros_like(hot128)

    loads[6].wait()
    both_here(5, fresh_kv)
    both_here(2, kv)
    odd = iota((HROWS, 1), 0) % 2 == 1
    own = [nt_dot(q16, kv[0, s]) for s in range(2)]
    scores = jnp.where(odd, own[1], own[0]) * SCALE
    length = jnp.where(odd, lengths[1], lengths[0])
    scores = jnp.where(iota((HROWS, CTX), 1) < length, scores, NEG)
    fresh_k = jnp.where(odd, fresh_kv[0, 1:2, :].astype(F32), fresh_kv[0, 0:1, :].astype(F32))
    fresh_v = jnp.where(odd, fresh_kv[1, 1:2, :].astype(F32), fresh_kv[1, 0:1, :].astype(F32))
    fresh = jnp.sum(qrows * fresh_k, axis=1, keepdims=True) * SCALE
    peak = jnp.maximum(jnp.max(scores, axis=1, keepdims=True), fresh)
    expo = jnp.exp(scores - peak)
    fresh_e = jnp.exp(fresh - peak)
    own_total = jnp.sum(expo, axis=1, keepdims=True) + fresh_e
    mixed = (
        dot(jnp.where(odd, 0.0, expo).astype(BF16), kv[1, 0])
        + dot(jnp.where(odd, expo, 0.0).astype(BF16), kv[1, 1])
        + fresh_e.astype(BF16).astype(F32) * fresh_v
    )
    own_peak = peak

    both_here(3, pkv)
    n = PER_X * HROWS
    k_i = iota((n, HD), 0) % HROWS
    seq = (iota((n, SEQS), 0) // HROWS) * 2 + iota((n, SEQS), 0) % 2
    for dx in ORDER1:
        group_here(0, qall, dx)
        base = first_of(dx)
        qs = qall[pl.ds(base, PER_X)].reshape(n, HD)
        member = seq + 2 * base == iota((n, SEQS), 1)
        times = nt_dot(jnp.where(member, 1.0, 0.0).astype(BF16), cntk[...])
        sc = nt_dot(qs, pkv[0].reshape(KEYS, HD)) * SCALE
        sc = jnp.where(times > 0.0, sc, NEG)
        m = jnp.max(sc, axis=1, keepdims=True)
        e = jnp.exp(sc - m) * times
        l = jnp.sum(e, axis=1, keepdims=True)
        o = dot(e.astype(BF16), pkv[1].reshape(KEYS, HD))
        some = l > 0.0
        safe = jnp.where(some, l, 1.0)
        o = o / safe
        lse = jnp.where(some, m + jnp.log(safe), NEG)
        diag = jnp.where(k_i == iota((n, HD), 1), lse, 0.0)
        across = jnp.sum(diag.reshape(PER_X, HROWS, HD), axis=1, keepdims=True)
        across = jnp.broadcast_to(across, (PER_X, HROWS, HD)).reshape(n, HD)
        hi = across.astype(BF16).astype(F32)
        mid = (across - hi).astype(BF16).astype(F32)
        lo = across - hi - mid
        tail = jnp.where(k_i == 12, hi, jnp.where(k_i == 13, mid, jnp.where(k_i == 14, lo, 0.0)))
        psend[pl.ds(base, PER_X)] = jnp.where(k_i < 12, o, tail).astype(BF16).reshape(PER_X, HROWS, HD)
        if dx == 0:
            prec[r] = psend[r]
        to_row(2, lambda peer: psend.at[peer], prec, dx)

    wait_for(recv_sem.at[RECV[1]], hrec, NC - 1)
    hot = jnp.sum(hrec[...], axis=0)
    hot128[0:EXPERTS, :] = hot
    u0, u1 = iota((128, 128), 0), iota((128, 128), 1)
    before = jnp.where((u0 < u1) & (u0 // BLOCK == u1 // BLOCK), 1.0, 0.0).astype(BF16)
    rank = dot(hot.astype(BF16), before)
    d_r, d_l = iota((ROWS, 128), 0), iota((ROWS, 128), 1)
    for e in range(EXPERTS):
        hit = (
            (hot[e : e + 1, :] > 0.0)
            & (rank[e : e + 1, :] == (d_r % CAP).astype(F32))
            & (d_l // BLOCK == d_r // CAP)
        )
        home = d_l % SEQS == e * BLOCK + d_r % BLOCK
        low = jnp.where(hit & (d_l < SEQS), 1.0, 0.0) + jnp.where(
            home & (d_l >= SEQS) & (d_r // BLOCK == 0), 1.0, 0.0
        )
        high = jnp.where(home & (d_r // BLOCK == 1 + d_l // SEQS), 1.0, 0.0)
        disp[e * ROWS : (e + 1) * ROWS, 0:128] = low.astype(BF16)
        disp[e * ROWS : (e + 1) * ROWS, 128:256] = high.astype(BF16)

    on_diag = iota((PER_X, HROWS, HD), 1) == iota((PER_X, HROWS, HD), 2)
    real = iota((PER_X, HROWS, 1), 1) < 12
    merged = [(own_peak, own_total, mixed)]
    for dx in ORDER2:
        group_here(2, prec, dx)
        parts = prec[pl.ds(first_of(dx), PER_X)].astype(F32)
        lrow = parts[:, 12:13, :] + parts[:, 13:14, :] + parts[:, 14:15, :]
        lse = jnp.sum(jnp.where(on_diag, jnp.broadcast_to(lrow, parts.shape), 0.0), axis=2, keepdims=True)
        lse = jnp.where(real, lse, NEG)
        top = jnp.max(lse, axis=0)
        w = jnp.exp(lse - top[None])
        w = jnp.where(lse > 0.5 * NEG, w, 0.0)
        merged.append((top, jnp.sum(w, axis=0), jnp.sum(w * parts, axis=0)))
    top = functools.reduce(jnp.maximum, [m for m, _, _ in merged])
    ws = [jnp.exp(m - top) for m, _, _ in merged]
    total = sum(w * l for w, (_, l, _) in zip(ws, merged))
    mixed = sum(w * o for w, (_, _, o) in zip(ws, merged))
    att = jnp.where(iota((HROWS, HD), 0) < 12, mixed / total, 0.0).astype(BF16)
    asend[...] = att
    aall[r] = att
    to_row(3, lambda peer: asend, aall)

    loads[15].wait()
    wait_for(recv_sem.at[RECV[3]], aall, NR - 1)
    for dx in range(NX):
        base = dx * PER_X
        picked = dot(sel[...], aall[pl.ds(base, PER_X)].reshape(PER_X * HROWS, HD)).astype(BF16)
        tokens = 2 * PER_X
        heads = jnp.concatenate([picked[g * tokens : (g + 1) * tokens] for g in range(GROUP)], axis=1)
        attended[pl.ds(pl.multiple_of(2 * base, tokens), tokens), :] = heads
    pbs[:, 0:WIDTH] = nt_dot(attended[...], wo[...])
    plain = pbs[...]
    with_hidden = plain + hplaced[...]
    lane = iota((SEQS, WPAD), 1)
    moved = [jnp.where(lane >= WIDTH, pltpu.roll(plain, WIDTH - 64 * i, 1), 0.0) for i in range(3)]
    stacked = jnp.concatenate([with_hidden] + moved, axis=0).astype(BF16)
    tsend[...] = dot(disp[...], stacked).astype(BF16).reshape(NC, ROWS, WPAD)
    trec[c] = tsend[c]
    to_col(4, lambda peer: tsend.at[peer], trec)

    wait_for(recv_sem.at[RECV[4]], trec, NC - 1)
    resid = jnp.sum(trec[...].astype(F32), axis=0)
    lane8 = iota((BLOCK, WPAD), 1)
    home = hpad[...]
    for i in range(3):
        piece = pltpu.roll(resid[i * BLOCK : (i + 1) * BLOCK, :], (64 * i + 64) % WPAD, 1)
        home = home + jnp.where(lane8 // 64 == i, piece, 0.0)
    hres[...] = home
    lane32 = iota((ROWS, WPAD), 1)
    squares = jnp.sum(jnp.where(lane32 < WIDTH, resid * resid, 0.0), axis=1, keepdims=True)
    x = resid * gpad[0:1, :]
    stats = dot(x[:, 0:WIDTH].astype(BF16), raug[...])
    stats = stats + jnp.where((lane32 >= WIDTH) & ((lane32 - WIDTH) % 16 == 8), squares, 0.0)
    hi = stats.astype(BF16).astype(F32)
    mid = (stats - hi).astype(BF16).astype(F32)
    lo = stats - hi - mid
    x = jnp.where(lane32 < WIDTH, x, jnp.where(lane32 < WIDTH + 16, hi, jnp.where(lane32 < WIDTH + 32, mid, jnp.where(lane32 < WIDTH + 48, lo, 0.0))))
    x = jnp.where(ry % 2 == 0, x, pltpu.roll(x, 64, 1)).astype(BF16)
    xsend[...] = x
    chip = r // NCORE
    xall[chip] = x
    to_chips(5, lambda peer: xsend, xall.at[chip])

    half_x = wx.at[pl.ds(0, D // NCORE // 2)]
    pltpu.make_async_copy(half_x, half_x, down_sem.at[3]).wait()
    pltpu.make_async_copy(half_x, half_x, down_sem.at[5]).wait()
    mine = disp[pl.ds(pl.multiple_of(c * ROWS, ROWS), ROWS), 0:128]
    mine = jnp.where(iota((ROWS, 128), 1) < SEQS, mine.astype(F32), 0.0)
    inner = jnp.zeros((ROWS, 4 * FSLICE), F32)
    even_st = jnp.zeros((ROWS, 128), F32)
    odd_st = jnp.zeros((ROWS, 128), F32)
    low_half = iota((ROWS, 128), 1) < 64
    for dx in NEAR_FIRST:
        wait_for(recv_sem.at[RECV[5] + dx], xall, NY - 1 if dx == 0 else NY)
        base = ((rx + dx) % NX) * NY
        pieces = []
        for j in range(NY // 2):
            even, odd_x = xall[base + 2 * j], xall[base + 2 * j + 1]
            pieces += [even[:, 0:128], jnp.where(low_half, even[:, 128:256], odd_x[:, 0:128]), odd_x[:, 128:256]]
            even_st = even_st + even[:, 128:256].astype(F32)
            odd_st = odd_st + odd_x[:, 0:128].astype(F32)
        rows = pl.ds(pl.multiple_of(base * WIDTH, NY * WIDTH), NY * WIDTH)
        inner = inner + dot(jnp.concatenate(pieces, axis=1), wx[rows, :])
    st = pltpu.roll(even_st, 64, 1) + odd_st
    stsend[...] = st
    to_partner(9, stsend, strecv, 0)
    insend[...] = inner.astype(BF16)
    to_partner(8, insend, inrecv, 0)
    pltpu.make_async_copy(strecv, strecv, recv_sem.at[RECV[9]]).wait()
    st = st + strecv[...]
    st = st + pltpu.roll(st, 112, 1) + pltpu.roll(st, 96, 1)
    lane128 = iota((ROWS, 128), 1)
    squares = jnp.sum(jnp.where(lane128 == 8, st, 0.0), axis=1, keepdims=True)
    inverse = lax.rsqrt(squares / D + EPS)
    pair = nt_dot(mine.astype(BF16), hot128[...].astype(BF16))
    logits = st * inverse
    own_logit = jnp.sum(jnp.where(lane128 == c, logits, 0.0), axis=1, keepdims=True)
    other = jnp.sum(jnp.where((pair > 0.0) & (lane128 != c), logits, 0.0), axis=1, keepdims=True)
    share = 1.0 / (1.0 + jnp.exp(other - own_logit))
    pltpu.make_async_copy(inrecv, inrecv, recv_sem.at[RECV[8]]).wait()
    theirs = inrecv[...].astype(F32)
    pair_of = [theirs[:, i * FSLICE : (i + 1) * FSLICE] for i in (1, 0, 3, 2)]
    inner = (inner + jnp.concatenate(pair_of, axis=1)) * inverse
    inner_gate, inner_up = inner[:, 0 : 2 * FSLICE], inner[:, 2 * FSLICE :]
    act = (inner_gate / (1.0 + jnp.exp(-inner_gate)) * inner_up * share).astype(BF16)
    half = wd.at[pl.ds(0, FSLICE)]
    pltpu.make_async_copy(half, half, down_sem.at[0]).wait()
    pltpu.make_async_copy(half, half, down_sem.at[2]).wait()
    for dx in FAR_FIRST:
        base = ((rx + dx) % NX) * NY
        y = dot(act, wd[:, pl.ds(pl.multiple_of(base * WPAD, NY * WPAD), NY * WPAD)])
        for j in range(NY):
            ypair[base + j] = y[:, j * WPAD : (j + 1) * WPAD].astype(BF16)
        if dx == 0:
            yrec[chip] = ypair[chip]
        to_chips(6, lambda peer: ypair.at[peer], yrec.at[chip], dx)

    ysum = jnp.zeros((ROWS, WPAD), F32)
    for dx in NEAR_FIRST:
        wait_for(recv_sem.at[RECV[6] + dx], yrec, NY - 1 if dx == 0 else NY)
        ysum = ysum + jnp.sum(yrec[chips_of(dx)].astype(F32), axis=0)
    ysum = jnp.where(rc == 0, ysum, pltpu.roll(ysum, WPAD - 64, 1))
    back = lax.dot_general(
        mine.astype(BF16), ysum.astype(BF16), (((0,), (0,)), ((), ())), preferred_element_type=F32
    )
    for i in range(NC):
        both = jnp.concatenate(
            [back[i * BLOCK : (i + 1) * BLOCK, 0:128], back[i * BLOCK : (i + 1) * BLOCK, 128:256]], axis=0
        )
        zsend[i] = both.astype(BF16)
    zrec[c] = zsend[c]
    to_col(7, lambda peer: zsend.at[peer], zrec)
    wait_for(recv_sem.at[RECV[7]], zrec, NC - 1)
    z = jnp.sum(zrec[...].astype(F32), axis=0)
    final = hres[...]
    out[:, 0:128] = (final[:, 0:128] + z[0:BLOCK]).astype(out.dtype)
    out[:, 128:WIDTH] = (final[:, 128:WIDTH] + z[BLOCK:, 0 : WIDTH - 128]).astype(out.dtype)

    wait_for(send_sem.at[0], qall, NR - 1)
    wait_for(send_sem.at[1], hrec, NC - 1)
    wait_for(send_sem.at[2], prec, NR - 1)
    wait_for(send_sem.at[3], aall, NR - 1)
    wait_for(send_sem.at[4], trec, NC - 1)
    wait_for(send_sem.at[5], yrec, CHIPS - 1)
    wait_for(send_sem.at[6], yrec, CHIPS - 1)
    pltpu.make_async_copy(inrecv, inrecv, send_sem.at[8]).wait()
    pltpu.make_async_copy(strecv, strecv, send_sem.at[9]).wait()
    pltpu.make_async_copy(half_x, half_x, down_sem.at[4]).wait()
    pltpu.make_async_copy(half, half, down_sem.at[1]).wait()
    wait_for(send_sem.at[7], zrec, NC - 1)


def body(
    hidden,
    queries,
    new_keys,
    new_values,
    cache_keys,
    cache_values,
    lengths,
    page_table,
    resident,
    prefix_keys,
    prefix_values,
    out_weight,
    norm_gain,
    router_weight,
    experts,
    gate_weight,
    up_weight,
    down_projection_weight,
):
    hbm = pl.BlockSpec(memory_space=pltpu.HBM)
    vmem = pl.BlockSpec(memory_space=pltpu.VMEM)
    operands = (
        lengths,
        resident.T,
        experts.T,
        hidden,
        queries,
        new_keys,
        new_values,
        page_table.T,
        norm_gain.reshape(1, WIDTH),
        router_weight.T,
        cache_keys,
        cache_values,
        prefix_keys,
        prefix_values,
        out_weight.T,
        gate_weight,
        up_weight,
        down_projection_weight,
    )
    return pl.pallas_call(
        kernel,
        out_shape=jax.ShapeDtypeStruct((BLOCK, WIDTH), BF16),
        in_specs=[hbm] * 18,
        out_specs=vmem,
        scratch_shapes=[
            pltpu.SMEM((2,), jnp.int32),
            pltpu.SMEM((SLOTS, NR), jnp.int32),
            pltpu.SMEM((2, BLOCK), jnp.int32),
            pltpu.VMEM((BLOCK, WIDTH), BF16),
            pltpu.VMEM((2, GROUP * HD), BF16),
            pltpu.VMEM((2, 2, HD), BF16),
            pltpu.VMEM((8, SEQS), jnp.int32),
            pltpu.VMEM((SLOTS, NR), jnp.int32),
            pltpu.VMEM((1, WIDTH), F32),
            pltpu.VMEM((EXPERTS, WIDTH), BF16),
            pltpu.VMEM((2, 2, CTX, HD), BF16),
            pltpu.VMEM((2, SLOTS, PAGE, HD), BF16),
            pltpu.VMEM((WIDTH, GROUP * HD), BF16),
            pltpu.VMEM((D // NCORE, 4 * FSLICE), BF16),
            pltpu.VMEM((NCORE * FSLICE, CHIPS * WPAD), BF16),
            pltpu.VMEM((HROWS, HD), BF16),
            pltpu.VMEM((NR, HROWS, HD), BF16),
            pltpu.VMEM((NR, HROWS, HD), BF16),
            pltpu.VMEM((NR, HROWS, HD), BF16),
            pltpu.VMEM((HROWS, HD), BF16),
            pltpu.VMEM((NR, HROWS, HD), BF16),
            pltpu.VMEM((NC, ROWS, WPAD), BF16),
            pltpu.VMEM((NC, ROWS, WPAD), BF16),
            pltpu.VMEM((ROWS, WPAD), BF16),
            pltpu.VMEM((CHIPS, ROWS, WPAD), BF16),
            pltpu.VMEM((ROWS, 4 * FSLICE), BF16),
            pltpu.VMEM((ROWS, 4 * FSLICE), BF16),
            pltpu.VMEM((ROWS, 128), F32),
            pltpu.VMEM((ROWS, 128), F32),
            pltpu.VMEM((CHIPS, ROWS, WPAD), BF16),
            pltpu.VMEM((CHIPS, ROWS, WPAD), BF16),
            pltpu.VMEM((NC, 2 * BLOCK, 128), BF16),
            pltpu.VMEM((NC, 2 * BLOCK, 128), BF16),
            pltpu.VMEM((EXPERTS, 128), F32),
            pltpu.VMEM((NC, EXPERTS, 128), F32),
            pltpu.VMEM((GROUP * 2 * PER_X, PER_X * HROWS), BF16),
            pltpu.VMEM((KEYS, SEQS), BF16),
            pltpu.VMEM((NC * ROWS, WPAD), BF16),
            pltpu.VMEM((128, 128), F32),
            pltpu.VMEM((WIDTH, WPAD), BF16),
            pltpu.VMEM((8, WPAD), F32),
            pltpu.VMEM((BLOCK, WPAD), F32),
            pltpu.VMEM((SEQS, WPAD), F32),
            pltpu.VMEM((SEQS, WPAD), F32),
            pltpu.VMEM((SEQS, GROUP * HD), BF16),
            pltpu.VMEM((BLOCK, WPAD), F32),
            pltpu.SemaphoreType.DMA((13,)),
            pltpu.SemaphoreType.DMA((6,)),
            pltpu.SemaphoreType.DMA((10,)),
            pltpu.SemaphoreType.DMA((25,)),
        ],
        compiler_params=pltpu.CompilerParams(
            collective_id=0, has_side_effects=True, vmem_limit_bytes=40 * 1024 * 1024
        ),
        name="layer",
    )(*[pltpu.with_memory_space_constraint(a, pltpu.HBM) for a in operands])


def solution(mesh):
    in_specs = (
        P("col", "row"),
        P("row", "col"),
        P("row", "col"),
        P("row", "col"),
        P("row", None, "col"),
        P("row", None, "col"),
        P("row"),
        P(),
        P(),
        P("row", None, None, "col"),
        P("row", None, None, "col"),
        P("col", "row"),
        P("row"),
        P("row", None),
        P("col", None),
        P("col", None, "row"),
        P("col", None, "row"),
        P("col", "row", None),
    )
    return jax.shard_map(body, mesh=mesh, in_specs=in_specs, out_specs=P("col", "row"), check_vma=False)
```
